32 devices in a mesh: dp: 2 (over core), context: 4 (over y, x), expert: 4 (over z).
Axes of the slice: x: 2, y: 2, z: 4, core: 2. Of those that a mesh axis runs over, the one named last changes fastest.
Arguments:
- hidden_in: bfloat16 [2, 2048, 2048], P('dp', ('context', 'expert')), may hold values from -6 to 6
- attn_gain: float32 [2048], replicated, may hold values from 0.5 to 1.5
- w_qkv: bfloat16 [3, 2048, 2048], P(None, None, 'expert'), may hold values from -0.125 to 0.125
- qk_gain: float32 [2, 2048], P(None, 'expert'), may hold values from 0.5 to 1.5
- w_out: bfloat16 [2048, 2048], P('expert'), may hold values from -0.375 to 0.375
- moe_gain: float32 [2048], replicated, may hold values from 0.5 to 1.5
- router: float32 [2048, 16], replicated, may hold values from -0.125 to 0.125
- w_gate: bfloat16 [16, 2048, 1024], P(('context', 'expert')), may hold values from -0.125 to 0.125
- w_up: bfloat16 [16, 2048, 1024], P(('context', 'expert')), may hold values from -0.125 to 0.125
- w_down: bfloat16 [16, 1024, 2048], P(('context', 'expert')), may hold values from -0.75 to 0.75
- expert_ids: int32 [2, 2048, 8], P('dp', ('context', 'expert')), may hold values from 0 to 15, all different within a row; in each aligned block of 128 rows (0 to 127, 128 to 255, ..., all dimensions but the last counted through in order) at most 96 rows name the same one
- grad_out: float32 [2, 2048, 2048], P('dp', ('context', 'expert')), may hold values from -6 to 6
Outputs:
- hidden_out: float32 [2, 2048, 2048], P('dp', ('context', 'expert'))
- grad_in: float32 [2, 2048, 2048], P('dp', ('context', 'expert'))
- attn_gain_grad: float32 [2048], replicated
- w_qkv_grad: float32 [3, 2048, 2048], P(None, None, 'expert')
- qk_gain_grad: float32 [2, 2048], P(None, 'expert')
- w_out_grad: float32 [2048, 2048], P('expert')
- moe_gain_grad: float32 [2048], replicated
- router_grad: float32 [2048, 16], replicated
- w_gate_grad: float32 [16, 2048, 1024], P(('context', 'expert'), 'dp')
- w_up_grad: float32 [16, 2048, 1024], P(('context', 'expert'), 'dp')
- w_down_grad: float32 [16, 1024, 2048], P(('context', 'expert'), 'dp')
The draws below stay inside these ranges and needn't reach their ends.
Inputs may be any that keep to these rules, and one draw needn't show every extreme that they name: `expert_ids`: each token names 8 different experts. In each aligned block of 128 tokens (the rows of one device) no expert is named more than 96 times, a bound that some block reaches.
All inputs are finite; a program needn't handle non-finite values.
Results may differ from the reference program's by a relative error of at most 0.023.
Values may be sent and summed in bfloat16 or wider, within the bound.
A program may use at most 256 MiB of HBM per device.

```python
import math
import jax
import jax.numpy as jnp
import numpy as np
from jax import lax

D = 2048
HEADS = 16
HEAD_DIM = 128
FF = 1024
TOPK = 8
TOK_DEV = 128
EXPERTS = 16
SEQ = 2048
SEQS = 2
CAP = 96
N_CONTEXT = 4


def shard_levels(own_key, extent, cuts, smallest, high):
    def one(position, shards_of):
        steps = jax.random.uniform(jax.random.fold_in(jax.random.fold_in(own_key, 6), position), (shards_of,), jnp.float32, smallest / len(cuts), high / len(cuts))
        return jnp.repeat(jnp.exp(steps), extent[position] // shards_of).reshape((-1,) + (1,) * (len(extent) - position - 1))

    gain = one(*cuts[0])
    for cut in cuts[1:]:
        gain = gain * one(*cut)
    return gain


def deal_out(key, own, number, rows, amount, top, most, slope):
    order = jax.random.permutation(key, amount)
    crowded, common = portions_of(amount, rows * top, most, slope, True), portions_of(amount, rows * top, most, slope, False)
    places = jnp.arange(amount)

    def named(lengths, offset_by):
        used = int((lengths > 0).sum())
        fixed = max(1, used // 4)
        moved = fixed + (places - fixed + offset_by * (used - fixed)) % max(1, amount - fixed)
        return jnp.zeros((amount,), jnp.int32).at[order[jnp.where(places < fixed, places, moved)]].set(jnp.asarray(lengths, jnp.int32))

    lengths = jnp.where(number % 4 == 0, named(crowded, number // 4), named(common, number - number // 4 - 1))
    mixed = jax.random.permutation(jax.random.fold_in(own, 3), amount)
    giver, receiver = mixed[0:amount // 2 * 2:2], mixed[1:amount // 2 * 2:2]
    room = jnp.minimum(lengths[giver] - 1, most - lengths[receiver]) // 2
    room = jnp.where((giver == order[0]) | (receiver == order[0]) | (lengths[receiver] == 0), 0, jnp.maximum(room, 0))
    moved = jax.random.randint(jax.random.fold_in(own, 4), (amount // 2,), 0, 1 << 20) % (room + 1)
    lengths = lengths.at[giver].add(-moved).at[receiver].add(moved)
    items = jnp.searchsorted(jnp.cumsum(lengths), jnp.arange(rows * top), side="right").astype(jnp.int32)
    grid = items.reshape(top, rows).T
    grid = grid[jax.random.permutation(jax.random.fold_in(own, 1), rows)]
    offset_by = jax.random.randint(jax.random.fold_in(own, 2), (rows, 1), 0, top)
    return jnp.take_along_axis(grid, (jnp.arange(top)[None, :] + offset_by) % top, axis=1)


def portions_of(number_of, total, most, lean, full):
    loads = [(1 << 20) // math.isqrt(rank ** lean) + 1 for rank in range(1, number_of + 1)]
    largest = most if full else min(most, max(-(-total // number_of), total * loads[0] // sum(loads)))
    least = 1 if total - largest >= number_of - 1 else 0
    counts, rest = [largest] + [least] * (number_of - 1), total - largest - least * (number_of - 1)
    while rest > 0:
        free = [i for i in range(1, number_of) if counts[i] < largest] or [i for i in range(1, number_of) if counts[i] < most]
        whole, left = sum([loads[i] for i in free]), rest
        for i in free:
            addition = min(most - counts[i], max(1, left * loads[i] // whole), rest)
            counts[i] = counts[i] + addition
            rest = rest - addition
    return np.array(counts)


def normal_values(rng, shape, spread, reach, pieces=(), kind=jnp.bfloat16):
    entries = jax.random.normal(rng, shape, jnp.float32) * spread
    if len(pieces) > 0:
        entries = shard_levels(rng, shape, pieces, -0.22, 0.18) * entries
    return jnp.clip(entries, min=-reach, max=reach).astype(kind)


def setup_inputs(seed: int = 0) -> dict:
    streams_of = jax.random.split(jax.random.key(seed), 13)
    hidden_in = normal_values(streams_of[0], (SEQS, SEQ, D), 1.0, 6.0, ((0, 2), (1, 16)))
    attn_gain = jnp.clip(1.0 + 0.1 * jax.random.normal(streams_of[1], (D,), jnp.float32), 0.5, 1.5)
    w_qkv = normal_values(streams_of[2], (3, D, HEADS * HEAD_DIM), D ** -0.5, 0.125, ((2, 4),))
    qk_gain = jnp.clip(1.0 + 0.1 * jax.random.normal(streams_of[3], (2, HEADS * HEAD_DIM), jnp.float32), 0.5, 1.5)
    w_out = normal_values(streams_of[4], (HEADS * HEAD_DIM, D), (HEADS * HEAD_DIM // 8) ** -0.5, 0.375, ((0, 4),))
    moe_gain = jnp.clip(1.0 + 0.1 * jax.random.normal(streams_of[5], (D,), jnp.float32), 0.5, 1.5)
    router = normal_values(streams_of[6], (D, EXPERTS), D ** -0.5, 0.125, (), jnp.float32)
    w_gate = normal_values(streams_of[7], (EXPERTS, D, FF), D ** -0.5, 0.125, ((0, 16),))
    w_up = normal_values(streams_of[8], (EXPERTS, D, FF), D ** -0.5, 0.125, ((0, 16),))
    w_down = normal_values(streams_of[9], (EXPERTS, FF, D), (FF // 16) ** -0.5, 0.75, ((0, 16),))
    expert_ids_keys = jax.random.split(jax.random.fold_in(streams_of[10], 1), SEQS * SEQ // TOK_DEV)
    expert_ids_turns = jax.random.permutation(jax.random.fold_in(streams_of[10], 3), SEQS * SEQ // TOK_DEV)
    expert_ids = jax.vmap(lambda own, number: deal_out(jax.random.fold_in(streams_of[10], 2), own, number, TOK_DEV, EXPERTS, TOPK, CAP, 2))(expert_ids_keys, expert_ids_turns).reshape((SEQS, SEQ, TOPK))
    grad_out = normal_values(streams_of[11], (SEQS, SEQ, D), 1.0, 6.0, ((0, 2), (1, 16)), jnp.float32)
    return {"hidden_in": hidden_in, "attn_gain": attn_gain, "w_qkv": w_qkv, "qk_gain": qk_gain, "w_out": w_out, "moe_gain": moe_gain, "router": router, "w_gate": w_gate, "w_up": w_up, "w_down": w_down, "expert_ids": expert_ids, "grad_out": grad_out}


norm_eps = 1e-05
rope_base = 10000.0
masked_score = -1e+30

def rms_scale(values, gain_vec):
    return values * lax.rsqrt(lax.optimization_barrier(jnp.mean(values * values, axis=-1, keepdims=True)) + norm_eps) * gain_vec

def folded_positions(row_ids, span_rows, block_total):
    block_id = row_ids // span_rows
    offset = row_ids % span_rows
    half_rows = span_rows // 2
    piece_id = jnp.where(offset < half_rows, block_id, 2 * block_total - 1 - block_id)
    return (piece_id * half_rows + offset % half_rows).astype(jnp.int32)

def qk_prep(pair_qk, gain_vec, places):
    row_total = pair_qk.shape[1]
    per_head = pair_qk.reshape(2, row_total, -1, HEAD_DIM)
    scaled = per_head * lax.rsqrt(lax.optimization_barrier(jnp.mean(per_head * per_head, axis=-1, keepdims=True)) + norm_eps)
    scaled = scaled * gain_vec.reshape(2, 1, -1, HEAD_DIM)
    half_dim = HEAD_DIM // 2
    frequency = rope_base ** (-2.0 * jnp.arange(half_dim, dtype=jnp.float32) / HEAD_DIM)
    angles = places.astype(jnp.float32)[:, None] * frequency[None, :]
    cosine = jnp.cos(angles)[None, :, None, :]
    sine_table = jnp.sin(angles)[None, :, None, :]
    first_half = scaled[..., :half_dim]
    second_half = scaled[..., half_dim:]
    turned = jnp.concatenate([first_half * cosine - second_half * sine_table, second_half * cosine + first_half * sine_table], axis=-1)
    return turned.reshape(2, row_total, -1)

def masked_scores(queries, key_heads, query_places, key_places, score_scale):
    scores = jnp.einsum('qhd,khd->hqk', queries.astype(jnp.float32), key_heads.astype(jnp.float32)) * score_scale
    return jnp.where(key_places[None, None, :] <= query_places[None, :, None], scores, masked_score)

def attend_forward(queries, key_heads, value_heads, query_places, key_places, score_scale):
    scores = masked_scores(queries, key_heads, query_places, key_places, score_scale)
    row_max = lax.optimization_barrier(jnp.max(scores, axis=-1, keepdims=True))
    log_total = row_max + jnp.log(lax.optimization_barrier(jnp.sum(jnp.exp(scores - row_max), axis=-1, keepdims=True)))
    prob_b = jnp.exp(scores - log_total).astype(jnp.bfloat16)
    result = jnp.einsum('hqk,khd->qhd', prob_b.astype(jnp.float32), value_heads.astype(jnp.float32))
    return (result.astype(jnp.bfloat16), log_total[..., 0])

def reference(hidden_in, attn_gain, w_qkv, qk_gain, w_out, moe_gain, router, w_gate, w_up, w_down, expert_ids, grad_out):
    span_rows = SEQ // N_CONTEXT
    places = folded_positions(jnp.arange(SEQ, dtype=jnp.int32), span_rows, N_CONTEXT)
    block_rows = min(512, span_rows)
    block_count = SEQ // block_rows
    score_scale = HEAD_DIM ** (-0.5)
    feat_width = HEADS * HEAD_DIM
    place_blocks = places.reshape(block_count, block_rows)
    stored = []
    resid_rows = []
    for seq_index in range(SEQS):
        tokens = hidden_in[seq_index].astype(jnp.float32)
        normed_b = rms_scale(tokens, attn_gain).astype(jnp.bfloat16)
        projected = jnp.stack([jnp.dot(normed_b, w_qkv[member], preferred_element_type=jnp.float32) for member in range(2)])
        value_rows = jnp.dot(normed_b, w_qkv[2], preferred_element_type=jnp.float32).astype(jnp.bfloat16)
        rotated = qk_prep(projected, qk_gain, places).astype(jnp.bfloat16)
        key_heads = rotated[1].reshape(SEQ, HEADS, HEAD_DIM)
        value_heads = value_rows.reshape(SEQ, HEADS, HEAD_DIM)
        query_blocks = rotated[0].reshape(block_count, block_rows, HEADS, HEAD_DIM)
        attended, log_totals = lax.map(lambda members: attend_forward(members[0], key_heads, value_heads, members[1], places, score_scale), (query_blocks, place_blocks))
        attended = attended.reshape(SEQ, feat_width)
        resid = tokens + jnp.dot(attended, w_out, preferred_element_type=jnp.float32)
        stored.append((tokens, normed_b, projected, query_blocks, key_heads, value_heads, attended, log_totals))
        resid_rows.append(resid)
    token_total = SEQS * SEQ
    resid_all = jnp.concatenate(resid_rows, axis=0)
    mixed_in = rms_scale(resid_all, moe_gain)
    logits = jnp.dot(mixed_in, router, precision=lax.Precision.HIGHEST, preferred_element_type=jnp.float32)
    gate_probs = jax.nn.softmax(logits, axis=-1)
    chosen = expert_ids.reshape(token_total, TOPK)
    weights = jnp.take_along_axis(gate_probs, chosen, axis=-1)
    weights_flat = weights.reshape(-1)
    expert_in = mixed_in.astype(jnp.bfloat16)
    upstream = grad_out.reshape(token_total, D)
    block_total = token_total // TOK_DEV
    per_block = TOK_DEV * TOPK
    flat_ids = chosen.reshape(block_total, per_block)
    onehot = (flat_ids[:, :, None] == jnp.arange(EXPERTS, dtype=jnp.int32)[None, None, :]).astype(jnp.int32)
    slot_index = lax.optimization_barrier(jnp.sum((jnp.cumsum(onehot, axis=1) - onehot) * onehot, axis=-1)).astype(jnp.int32)
    column = (jnp.arange(block_total, dtype=jnp.int32)[:, None] * CAP + slot_index).astype(jnp.int32)
    assign_index = jnp.arange(block_total * per_block, dtype=jnp.int32).reshape(block_total, per_block)
    slot_table = jnp.full((EXPERTS, block_total * CAP), -1, dtype=jnp.int32).at[flat_ids, column].set(assign_index)

    def expert_step(totals, members):
        mixed_sum, grad_sum, weight_grad = totals
        table_row, gate_w, up_w, down_w = members
        is_valid = table_row >= 0
        safe_index = jnp.where(is_valid, table_row, 0).astype(jnp.int32)
        token_row = (safe_index // TOPK).astype(jnp.int32)
        row_block = jnp.where(is_valid[:, None], expert_in[token_row], jnp.zeros((), jnp.bfloat16))
        factor = jnp.where(is_valid, weights_flat[safe_index], 0.0)
        gate_pre = jnp.dot(row_block, gate_w, preferred_element_type=jnp.float32)
        up_pre = jnp.dot(row_block, up_w, preferred_element_type=jnp.float32)
        sigmoid_g = jax.nn.sigmoid(gate_pre)
        activated = gate_pre * sigmoid_g
        hidden = (activated * up_pre).astype(jnp.bfloat16)
        out_float = jnp.dot(hidden, down_w, preferred_element_type=jnp.float32).astype(jnp.bfloat16).astype(jnp.float32)
        incoming = upstream[token_row]
        mixed_sum = mixed_sum.at[token_row].add(factor[:, None] * out_float)
        weight_grad = weight_grad.at[safe_index].add(jnp.where(is_valid, lax.optimization_barrier(jnp.sum(out_float * incoming, axis=-1)), 0.0))
        grad_outb = (factor[:, None] * incoming).astype(jnp.bfloat16)
        grad_hidden = jnp.dot(grad_outb, down_w.T, preferred_element_type=jnp.float32)
        down_grad = jnp.dot(hidden.T, grad_outb, preferred_element_type=jnp.float32)
        grad_gate = (grad_hidden * up_pre * sigmoid_g * (1.0 + gate_pre * (1.0 - sigmoid_g))).astype(jnp.bfloat16)
        grad_up = (grad_hidden * activated).astype(jnp.bfloat16)
        gate_grad = jnp.dot(row_block.T, grad_gate, preferred_element_type=jnp.float32)
        up_grad = jnp.dot(row_block.T, grad_up, preferred_element_type=jnp.float32)
        grad_rows = (jnp.dot(grad_gate, gate_w.T, preferred_element_type=jnp.float32) + jnp.dot(grad_up, up_w.T, preferred_element_type=jnp.float32)).astype(jnp.bfloat16)
        grad_sum = grad_sum.at[token_row].add(grad_rows.astype(jnp.float32))
        return ((mixed_sum, grad_sum, weight_grad), (gate_grad, up_grad, down_grad))
    initial = (jnp.zeros((token_total, D), jnp.float32), jnp.zeros((token_total, D), jnp.float32), jnp.zeros((token_total * TOPK,), jnp.float32))
    (moe_out, mixed_grad_experts, weight_grads), (gate_grads, up_grads, down_grads) = lax.scan(expert_step, initial, (slot_table, w_gate, w_up, w_down))
    hidden_out = (resid_all + moe_out).reshape(SEQS, SEQ, D)
    d_weights = weight_grads.reshape(token_total, TOPK)
    picked = chosen[:, :, None] == jnp.arange(EXPERTS, dtype=jnp.int32)[None, None, :]
    d_gates = lax.optimization_barrier(jnp.sum(jnp.where(picked, d_weights[:, :, None], 0.0), axis=1))
    d_logits = gate_probs * (d_gates - lax.optimization_barrier(jnp.sum(gate_probs * d_gates, axis=-1, keepdims=True)))
    router_grad = jnp.dot(mixed_in.T, d_logits, precision=lax.Precision.HIGHEST, preferred_element_type=jnp.float32)
    d_mixed = mixed_grad_experts + jnp.dot(d_logits, router.T, precision=lax.Precision.HIGHEST, preferred_element_type=jnp.float32)
    _, second_pull = jax.vjp(rms_scale, resid_all, moe_gain)
    resid_part, moe_gain_grad = second_pull(d_mixed)
    d_resid = (upstream + resid_part).reshape(SEQS, SEQ, D)
    qkv_grad = jnp.zeros((3, D, feat_width), jnp.float32)
    out_grad = jnp.zeros((feat_width, D), jnp.float32)
    qk_grad = jnp.zeros((2, feat_width), jnp.float32)
    attn_grad = jnp.zeros((D,), jnp.float32)
    grad_rows_all = []
    for seq_index in range(SEQS):
        tokens, normed_b, projected, query_blocks, key_heads, value_heads, attended, log_totals = stored[seq_index]
        resid_b = d_resid[seq_index].astype(jnp.bfloat16)
        out_grad = out_grad + jnp.dot(attended.T, resid_b, preferred_element_type=jnp.float32)
        d_attended = jnp.dot(resid_b, w_out.T, preferred_element_type=jnp.float32).astype(jnp.bfloat16)
        grad_blocks = d_attended.reshape(block_count, block_rows, HEADS, HEAD_DIM)

        def backward_block(totals, members):
            key_acc, value_acc = totals
            query_blk, grad_blk, place_blk, total_blk = members
            scores = masked_scores(query_blk, key_heads, place_blk, places, score_scale)
            prob_exact = jnp.exp(scores - total_blk[:, :, None])
            prob_b = prob_exact.astype(jnp.bfloat16)
            d_probs = jnp.einsum('qhd,khd->hqk', grad_blk.astype(jnp.float32), value_heads.astype(jnp.float32))
            row_dot = lax.optimization_barrier(jnp.sum(prob_exact * d_probs, axis=-1, keepdims=True))
            d_scores = (prob_exact * (d_probs - row_dot) * score_scale).astype(jnp.bfloat16)
            d_query = jnp.einsum('hqk,khd->qhd', d_scores.astype(jnp.float32), key_heads.astype(jnp.float32))
            key_acc = key_acc + jnp.einsum('hqk,qhd->khd', d_scores.astype(jnp.float32), query_blk.astype(jnp.float32))
            value_acc = value_acc + jnp.einsum('hqk,qhd->khd', prob_b.astype(jnp.float32), grad_blk.astype(jnp.float32))
            return ((key_acc, value_acc), d_query)
        zero_heads = jnp.zeros((SEQ, HEADS, HEAD_DIM), jnp.float32)
        (key_acc, value_acc), d_queries = lax.scan(backward_block, (zero_heads, zero_heads), (query_blocks, grad_blocks, place_blocks, log_totals))
        d_rotated = jnp.stack([d_queries.reshape(SEQ, feat_width), key_acc.reshape(SEQ, feat_width)])
        _, prep_pull = jax.vjp(lambda pair_qk, gain_vec: qk_prep(pair_qk, gain_vec, places), projected, qk_gain)
        d_pair, qk_part = prep_pull(d_rotated)
        qk_grad = qk_grad + qk_part
        d_proj = jnp.concatenate([d_pair, value_acc.reshape(1, SEQ, feat_width)], axis=0).astype(jnp.bfloat16)
        qkv_grad = qkv_grad + jnp.stack([jnp.dot(normed_b.T, d_proj[member], preferred_element_type=jnp.float32) for member in range(3)])
        d_normed = jnp.dot(d_proj[0], w_qkv[0].T, preferred_element_type=jnp.float32)
        d_normed = d_normed + jnp.dot(d_proj[1], w_qkv[1].T, preferred_element_type=jnp.float32)
        d_normed = d_normed + jnp.dot(d_proj[2], w_qkv[2].T, preferred_element_type=jnp.float32)
        _, first_pull = jax.vjp(rms_scale, tokens, attn_gain)
        token_part, gain_part = first_pull(d_normed)
        attn_grad = attn_grad + gain_part
        grad_rows_all.append(d_resid[seq_index] + token_part)
    grad_in = jnp.stack(grad_rows_all)
    return (hidden_out, grad_in, attn_grad, qkv_grad, qk_grad, out_grad, moe_gain_grad, router_grad, gate_grads, up_grads, down_grads)
```

```python
import functools

import jax
import jax.numpy as jnp
from jax import lax
from jax.experimental import pallas as pl
from jax.experimental.pallas import tpu as pltpu
from jax.sharding import PartitionSpec as P

HEAD_DIM = 128


norm_eps = 1e-05
rope_base = 10000.0
masked_score = -1e30


def rms_scale(values, gain_vec):
    return (
        values * lax.rsqrt(jnp.mean(values * values, axis=-1, keepdims=True) + norm_eps) * gain_vec
    )


def folded_positions(row_ids, span_rows, block_total):
    block_id = row_ids // span_rows
    offset = row_ids % span_rows
    half_rows = span_rows // 2
    piece_id = jnp.where(offset < half_rows, block_id, 2 * block_total - 1 - block_id)
    return piece_id * half_rows + offset % half_rows


def qk_prep(pair_qk, gain_vec, places):
    row_total = pair_qk.shape[1]
    per_head = pair_qk.reshape(2, row_total, -1, HEAD_DIM)
    scaled = per_head * lax.rsqrt(jnp.mean(per_head * per_head, axis=-1, keepdims=True) + norm_eps)
    scaled = scaled * gain_vec.reshape(2, 1, -1, HEAD_DIM)
    half_dim = HEAD_DIM // 2
    frequency = rope_base ** (-2.0 * jnp.arange(half_dim, dtype=jnp.float32) / HEAD_DIM)
    angles = places.astype(jnp.float32)[:, None] * frequency[None, :]
    cosine = jnp.cos(angles)[None, :, None, :]
    sine_table = jnp.sin(angles)[None, :, None, :]
    first_half = scaled[..., :half_dim]
    second_half = scaled[..., half_dim:]
    turned = jnp.concatenate(
        [
            first_half * cosine - second_half * sine_table,
            second_half * cosine + first_half * sine_table,
        ],
        axis=-1,
    )
    return turned.reshape(2, row_total, -1)


def masked_scores(queries, key_heads, query_places, key_places, score_scale):
    scores = (
        jnp.einsum("qhd,khd->hqk", queries, key_heads, preferred_element_type=jnp.float32)
        * score_scale
    )
    return jnp.where(key_places[None, None, :] <= query_places[None, :, None], scores, masked_score)


def contract(left, right, left_dim, right_dim):
    return lax.dot_general(
        left, right, (((left_dim,), (right_dim,)), ((), ())), preferred_element_type=jnp.float32
    )


def nt_dot(left, right):
    return lax.dot_general(
        left, right, (((1,), (1,)), ((), ())), preferred_element_type=jnp.float32
    )


def tn_dot(left, right):
    return lax.dot_general(
        left, right, (((0,), (0,)), ((), ())), preferred_element_type=jnp.float32
    )


def nn_dot(left, right):
    return jnp.dot(left, right, preferred_element_type=jnp.float32)


def as_row(column):
    wide = jnp.broadcast_to(column, (column.shape[0], 128))
    return jnp.transpose(wide)[0:1]


def piece_start(piece, blocks, half):
    return jnp.where(
        piece < blocks, piece * 2 * half, (2 * blocks - 1 - piece) * 2 * half + half
    )


def attend_kernel(blocks, half, place_ref, q_ref, k_ref, v_ref, out_ref, lse_ref):
    mine = place_ref[0]
    scale = HEAD_DIM ** (-0.5)
    row_ids = lax.broadcasted_iota(jnp.int32, (half, half), 0)
    col_ids = lax.broadcasted_iota(jnp.int32, (half, half), 1)
    for part in range(2):
        own = mine if part == 0 else 2 * blocks - 1 - mine
        rows = pl.ds(part * half, half)
        queries = q_ref[rows, :]

        def tile(piece):
            start = pl.multiple_of(piece_start(piece, blocks, half), half)
            scores = nt_dot(queries, k_ref[pl.ds(start, half), :]) * scale
            return jnp.exp(scores), v_ref[pl.ds(start, half), :]

        def step(piece, carry):
            total, acc = carry
            prob, value = tile(piece)
            total = total + jnp.sum(prob, axis=-1, keepdims=True)
            return total, acc + nn_dot(prob.astype(jnp.bfloat16), value)

        total, acc = lax.fori_loop(
            0,
            own,
            step,
            (jnp.zeros((half, 1), jnp.float32), jnp.zeros((half, HEAD_DIM), jnp.float32)),
        )
        prob, value = tile(own)
        prob = jnp.where(col_ids <= row_ids, prob, 0.0)
        total = total + jnp.sum(prob, axis=-1, keepdims=True)
        acc = acc + nn_dot(prob.astype(jnp.bfloat16), value)
        out_ref[rows, :] = (acc / total).astype(jnp.bfloat16)
        lse_ref[0, :, pl.ds(part * half, half)] = as_row(jnp.log(total))


def attend(place, queries, keys, values, blocks):
    span, feat = queries.shape
    seq = keys.shape[0]
    heads = feat // HEAD_DIM
    half = span // 2
    head_block = lambda rows: pl.BlockSpec((rows, HEAD_DIM), lambda h: (0, h))
    return pl.pallas_call(
        functools.partial(attend_kernel, blocks, half),
        grid=(heads,),
        in_specs=[
            pl.BlockSpec(memory_space=pltpu.SMEM),
            head_block(span),
            head_block(seq),
            head_block(seq),
        ],
        out_specs=[head_block(span), pl.BlockSpec((1, 1, span), lambda h: (h, 0, 0))],
        out_shape=[
            jax.ShapeDtypeStruct((span, feat), jnp.bfloat16),
            jax.ShapeDtypeStruct((heads, 1, span), jnp.float32),
        ],
        name="attend",
    )(place, queries, keys, values)


def attend_back_kernel(
    blocks, half, place_ref, q_ref, g_ref, o_ref, lse_ref, k_ref, v_ref,
    dq_ref, dk_ref, dv_ref, dk_acc, dv_acc,
):
    mine = place_ref[0]
    scale = HEAD_DIM ** (-0.5)
    key_ids = lax.broadcasted_iota(jnp.int32, (half, half), 0)
    query_ids = lax.broadcasted_iota(jnp.int32, (half, half), 1)
    dk_acc[...] = jnp.zeros_like(dk_acc)
    dv_acc[...] = jnp.zeros_like(dv_acc)
    for part in range(2):
        own = mine if part == 0 else 2 * blocks - 1 - mine
        rows = pl.ds(part * half, half)
        queries = q_ref[rows, :]
        grads = g_ref[rows, :]
        lse = lse_ref[0, :, pl.ds(part * half, half)]
        row_dot = as_row(
            jnp.sum(
                grads.astype(jnp.float32) * o_ref[rows, :].astype(jnp.float32),
                axis=-1,
                keepdims=True,
            )
        )

        def tile(piece, masked, acc):
            start = pl.multiple_of(piece_start(piece, blocks, half), half)
            place = pl.ds(start, half)
            keys = k_ref[place, :]
            prob = jnp.exp(nt_dot(keys, queries) * scale - lse)
            if masked:
                prob = jnp.where(key_ids <= query_ids, prob, 0.0)
            d_prob = nt_dot(v_ref[place, :], grads)
            d_score = (prob * (d_prob - row_dot) * scale).astype(jnp.bfloat16)
            dv_acc[place, :] += nn_dot(prob.astype(jnp.bfloat16), grads)
            dk_acc[place, :] += nn_dot(d_score, queries)
            return acc + tn_dot(d_score, keys)

        acc = lax.fori_loop(
            0,
            own,
            lambda piece, acc: tile(piece, False, acc),
            jnp.zeros((half, HEAD_DIM), jnp.float32),
        )
        dq_ref[rows, :] = tile(own, True, acc)
    dk_ref[...] = dk_acc[...].astype(jnp.bfloat16)
    dv_ref[...] = dv_acc[...].astype(jnp.bfloat16)


def attend_back(place, queries, grads, attended, lse, keys, values, blocks):
    span, feat = queries.shape
    seq = keys.shape[0]
    heads = feat // HEAD_DIM
    half = span // 2
    head_block = lambda rows: pl.BlockSpec((rows, HEAD_DIM), lambda h: (0, h))
    return pl.pallas_call(
        functools.partial(attend_back_kernel, blocks, half),
        grid=(heads,),
        in_specs=[
            pl.BlockSpec(memory_space=pltpu.SMEM),
            head_block(span),
            head_block(span),
            head_block(span),
            pl.BlockSpec((1, 1, span), lambda h: (h, 0, 0)),
            head_block(seq),
            head_block(seq),
        ],
        out_specs=[head_block(span), head_block(seq), head_block(seq)],
        out_shape=[
            jax.ShapeDtypeStruct((span, feat), jnp.float32),
            jax.ShapeDtypeStruct((seq, feat), jnp.bfloat16),
            jax.ShapeDtypeStruct((seq, feat), jnp.bfloat16),
        ],
        scratch_shapes=[pltpu.VMEM((seq, HEAD_DIM), jnp.float32)] * 2,
        name="attend_back",
    )(place, queries, grads, attended, lse, keys, values)


def split_pair(values):
    upper = values.astype(jnp.bfloat16)
    lower = (values - upper.astype(jnp.float32)).astype(jnp.bfloat16)
    return upper, lower


TOKEN_AXES = ("context", "expert")


def fast_device(
    hidden_in,
    attn_gain,
    w_qkv,
    qk_gain,
    w_out,
    moe_gain,
    router,
    w_gate,
    w_up,
    w_down,
    expert_ids,
    grad_out,
):
    tokens = hidden_in[0].astype(jnp.float32)
    upstream = grad_out[0]
    tok_count, model_width = tokens.shape
    context_size = lax.axis_size("context")
    expert_size = lax.axis_size("expert")
    expert_count = router.shape[1]
    span_rows = tok_count * expert_size
    context_index = lax.axis_index("context")
    own_expert = context_index * expert_size + lax.axis_index("expert")
    place = jnp.full((1,), context_index, jnp.int32)
    local_places = folded_positions(
        context_index * span_rows + jnp.arange(span_rows, dtype=jnp.int32), span_rows, context_size
    )

    normed_b = rms_scale(tokens, attn_gain).astype(jnp.bfloat16)
    gathered_in = lax.all_gather(normed_b, "expert", axis=0, tiled=True)
    all_upstream = lax.all_gather(
        upstream.astype(jnp.bfloat16), TOKEN_AXES, axis=0, tiled=True
    )
    projected = jnp.einsum(
        "rd,kdf->krf", gathered_in, w_qkv[:2], preferred_element_type=jnp.float32
    )
    value_local = nn_dot(gathered_in, w_qkv[2]).astype(jnp.bfloat16)

    def prep_local(pair_qk, gain_vec):
        return qk_prep(pair_qk, gain_vec, local_places)

    rotated = prep_local(projected, qk_gain).astype(jnp.bfloat16)
    feat_width = projected.shape[2]
    keys_all = lax.all_gather(rotated[1], "context", axis=0, tiled=True)
    values_all = lax.all_gather(value_local, "context", axis=0, tiled=True)
    attended, lse = attend(place, rotated[0], keys_all, values_all, context_size)
    branch_out = lax.psum_scatter(
        nn_dot(attended, w_out).astype(jnp.bfloat16), "expert", scatter_dimension=0, tiled=True
    ).astype(jnp.float32)
    resid = tokens + branch_out
    mixed_in = rms_scale(resid, moe_gain)
    logits = jnp.dot(
        mixed_in, router, precision=lax.Precision.HIGHEST, preferred_element_type=jnp.float32
    )
    gate_probs = jax.nn.softmax(logits, axis=-1)
    chosen = expert_ids[0]
    picked = jnp.any(
        chosen[:, :, None] == jnp.arange(expert_count, dtype=jnp.int32)[None, None, :], axis=1
    )
    weights = jnp.where(picked, gate_probs, 0.0)
    expert_in = mixed_in.astype(jnp.bfloat16)
    pad = jnp.zeros((tok_count, 128 - 2 * expert_count), jnp.bfloat16)
    sending = jnp.concatenate([expert_in, *split_pair(weights), pad], axis=1)
    arrived = lax.all_gather(sending, TOKEN_AXES, axis=0, tiled=True)
    rows = arrived[:, :model_width]
    pairs = arrived[:, model_width:].astype(jnp.float32)
    lane = jnp.arange(128, dtype=jnp.int32)[None, :]
    mine = (lane == own_expert) | (lane == own_expert + expert_count)
    factor = jnp.sum(jnp.where(mine, pairs, 0.0), axis=1, keepdims=True)
    gate_pre = nn_dot(rows, w_gate[0])
    up_pre = nn_dot(rows, w_up[0])
    back_hidden = nt_dot(all_upstream, w_down[0])
    sigmoid_g = jax.nn.sigmoid(gate_pre)
    activated = gate_pre * sigmoid_g
    hidden = activated * up_pre
    d_weight = jnp.sum(hidden * back_hidden, axis=1, keepdims=True)
    hidden_w = (factor * hidden).astype(jnp.bfloat16)
    grad_hidden = factor * back_hidden
    grad_gate = (grad_hidden * up_pre * sigmoid_g * (1.0 + gate_pre * (1.0 - sigmoid_g))).astype(
        jnp.bfloat16
    )
    grad_up = (grad_hidden * activated).astype(jnp.bfloat16)
    grad_rows = (nt_dot(grad_gate, w_gate[0]) + nt_dot(grad_up, w_up[0])).astype(jnp.bfloat16)
    upper, lower = split_pair(d_weight)
    d_pairs = jnp.where(lane == own_expert, upper, jnp.zeros((), jnp.bfloat16)) + jnp.where(
        lane == own_expert + expert_count, lower, jnp.zeros((), jnp.bfloat16)
    )
    returned = lax.psum_scatter(
        jnp.concatenate([grad_rows, d_pairs], axis=1),
        TOKEN_AXES,
        scatter_dimension=0,
        tiled=True,
    ).astype(jnp.float32)
    hidden_out = resid + lax.psum_scatter(
        nn_dot(hidden_w, w_down[0]).astype(jnp.bfloat16),
        TOKEN_AXES,
        scatter_dimension=0,
        tiled=True,
    ).astype(jnp.float32)

    def over_sequences(grad):
        return lax.psum_scatter(
            grad.astype(jnp.bfloat16)[None], "dp", scatter_dimension=1, tiled=True
        ).astype(jnp.float32)

    gate_sum = over_sequences(tn_dot(rows, grad_gate))
    up_sum = over_sequences(tn_dot(rows, grad_up))
    down_sum = over_sequences(tn_dot(hidden_w, all_upstream))

    d_weights = (
        returned[:, model_width : model_width + expert_count]
        + returned[:, model_width + expert_count : model_width + 2 * expert_count]
    )
    d_gates = jnp.where(picked, d_weights, 0.0)
    d_logits = gate_probs * (d_gates - jnp.sum(gate_probs * d_gates, axis=-1, keepdims=True))
    router_part = lax.dot_general(
        mixed_in,
        d_logits,
        (((0,), (0,)), ((), ())),
        precision=lax.Precision.HIGHEST,
        preferred_element_type=jnp.float32,
    )
    d_mixed = returned[:, :model_width] + lax.dot_general(
        d_logits,
        router,
        (((1,), (1,)), ((), ())),
        precision=lax.Precision.HIGHEST,
        preferred_element_type=jnp.float32,
    )
    _, second_pull = jax.vjp(rms_scale, resid, moe_gain)
    resid_part, moe_gain_part = second_pull(d_mixed)
    d_resid = upstream + resid_part
    grad_gathered = lax.all_gather(
        d_resid.astype(jnp.bfloat16), "expert", axis=0, tiled=True
    )
    out_grad = tn_dot(attended, grad_gathered)
    d_attended = nt_dot(grad_gathered, w_out).astype(jnp.bfloat16)
    d_queries, key_part, value_part = attend_back(
        place, rotated[0], d_attended, attended, lse, keys_all, values_all, context_size
    )
    key_grad = lax.psum_scatter(
        key_part, "context", scatter_dimension=0, tiled=True
    ).astype(jnp.float32)
    value_grad = lax.psum_scatter(
        value_part, "context", scatter_dimension=0, tiled=True
    ).astype(jnp.float32)
    d_rotated = jnp.stack([d_queries, key_grad])
    _, prep_pull = jax.vjp(prep_local, projected, qk_gain)
    d_pair, qk_part = prep_pull(d_rotated)
    d_proj = jnp.concatenate([d_pair, value_grad[None]], axis=0).astype(jnp.bfloat16)
    qkv_grad = jnp.einsum("rd,krf->kdf", gathered_in, d_proj, preferred_element_type=jnp.float32)
    d_normed = lax.psum_scatter(
        jnp.einsum("krf,kdf->rd", d_proj, w_qkv, preferred_element_type=jnp.float32).astype(
            jnp.bfloat16
        ),
        "expert",
        scatter_dimension=0,
        tiled=True,
    ).astype(jnp.float32)
    _, first_pull = jax.vjp(rms_scale, tokens, attn_gain)
    token_part, attn_gain_part = first_pull(d_normed)
    grad_in = d_resid + token_part
    qkv_sum, out_sum, qk_sum = (
        lax.psum(qkv_grad.astype(jnp.bfloat16), ("dp", "context")).astype(jnp.float32),
        lax.psum(out_grad.astype(jnp.bfloat16), ("dp", "context")).astype(jnp.float32),
        lax.psum(qk_part.astype(jnp.bfloat16), ("dp", "context")).astype(jnp.float32),
    )
    attn_sum, moe_sum, router_sum = lax.psum(
        (attn_gain_part, moe_gain_part, router_part), ("dp", "context", "expert")
    )
    return (
        hidden_out[None],
        grad_in[None],
        attn_sum,
        qkv_sum,
        qk_sum,
        out_sum,
        moe_sum,
        router_sum,
        gate_sum,
        up_sum,
        down_sum,
    )


def portable_device(
    hidden_in,
    attn_gain,
    w_qkv,
    qk_gain,
    w_out,
    moe_gain,
    router,
    w_gate,
    w_up,
    w_down,
    expert_ids,
    grad_out,
):
    tokens = hidden_in[0].astype(jnp.float32)
    tok_count = tokens.shape[0]
    model_width = tokens.shape[1]
    context_size = lax.axis_size("context")
    expert_size = lax.axis_size("expert")
    span_rows = tok_count * expert_size
    seq_rows = span_rows * context_size
    context_index = lax.axis_index("context")
    local_places = folded_positions(
        context_index * span_rows + jnp.arange(span_rows, dtype=jnp.int32), span_rows, context_size
    )
    key_places = folded_positions(jnp.arange(seq_rows, dtype=jnp.int32), span_rows, context_size)
    score_scale = HEAD_DIM ** (-0.5)
    normed_b = rms_scale(tokens, attn_gain).astype(jnp.bfloat16)
    gathered_in = lax.all_gather(normed_b, "expert", axis=0, tiled=True)
    projected = jnp.einsum(
        "rd,kdf->krf", gathered_in, w_qkv[:2], preferred_element_type=jnp.float32
    )
    value_local = jnp.dot(gathered_in, w_qkv[2], preferred_element_type=jnp.float32).astype(
        jnp.bfloat16
    )
    feat_width = projected.shape[2]
    heads_here = feat_width // HEAD_DIM

    def prep_local(pair_qk, gain_vec):
        return qk_prep(pair_qk, gain_vec, local_places)

    rotated = prep_local(projected, qk_gain).astype(jnp.bfloat16)
    keys_all, values_all = (
        lax.all_gather(rotated[1], "context", axis=0, tiled=True),
        lax.all_gather(value_local, "context", axis=0, tiled=True),
    )
    key_heads = keys_all.reshape(seq_rows, heads_here, HEAD_DIM)
    value_heads = values_all.reshape(seq_rows, heads_here, HEAD_DIM)
    block_rows = min(512, span_rows)
    block_count = span_rows // block_rows
    key_count = seq_rows // block_rows
    key_lowest = jnp.min(key_places.reshape(key_count, block_rows), axis=1)
    query_blocks = rotated[0].reshape(block_count, block_rows, heads_here, HEAD_DIM)
    place_blocks = local_places.reshape(block_count, block_rows)

    def key_piece(kb):
        start = kb * block_rows
        return (
            lax.dynamic_slice_in_dim(key_heads, start, block_rows, 0),
            lax.dynamic_slice_in_dim(value_heads, start, block_rows, 0),
            lax.dynamic_slice_in_dim(key_places, start, block_rows, 0),
        )

    def attend_blocks(members):
        queries, query_places = members
        query_top = jnp.max(query_places)

        def stat_step(kb, carry):

            def stat_live(state):
                run_max, run_sum = state
                key_blk, value_blk, kplace = key_piece(kb)
                scores = masked_scores(queries, key_blk, query_places, kplace, score_scale)
                new_max = jnp.maximum(run_max, jnp.max(scores, axis=-1))
                new_sum = run_sum * jnp.exp(run_max - new_max) + jnp.sum(
                    jnp.exp(scores - new_max[..., None]), axis=-1
                )
                return (new_max, new_sum)

            return lax.cond(key_lowest[kb] <= query_top, stat_live, lambda state: state, carry)

        start_stat = (
            jnp.full((heads_here, block_rows), masked_score, jnp.float32),
            jnp.zeros((heads_here, block_rows), jnp.float32),
        )
        run_max, run_sum = lax.fori_loop(0, key_count, stat_step, start_stat)
        log_total = run_max + jnp.log(run_sum)

        def value_step(kb, acc):

            def value_live(total):
                key_blk, value_blk, kplace = key_piece(kb)
                scores = masked_scores(queries, key_blk, query_places, kplace, score_scale)
                prob_b = jnp.exp(scores - log_total[..., None]).astype(jnp.bfloat16)
                return total + jnp.einsum(
                    "hqk,khd->qhd", prob_b, value_blk, preferred_element_type=jnp.float32
                )

            return lax.cond(key_lowest[kb] <= query_top, value_live, lambda total: total, acc)

        result = lax.fori_loop(
            0, key_count, value_step, jnp.zeros((block_rows, heads_here, HEAD_DIM), jnp.float32)
        )
        return (result.astype(jnp.bfloat16), log_total)

    attended, log_totals = lax.map(attend_blocks, (query_blocks, place_blocks))
    attended = attended.reshape(span_rows, feat_width)
    piece_rows = attended
    branch_out = lax.psum_scatter(
        jnp.dot(piece_rows, w_out, preferred_element_type=jnp.float32).astype(jnp.bfloat16),
        "expert",
        scatter_dimension=0,
        tiled=True,
    ).astype(jnp.float32)
    resid = tokens + branch_out
    mixed_in = rms_scale(resid, moe_gain)
    logits = jnp.dot(
        mixed_in, router, precision=lax.Precision.HIGHEST, preferred_element_type=jnp.float32
    )
    gate_probs = jax.nn.softmax(logits, axis=-1)
    chosen = expert_ids[0]
    top_count = chosen.shape[1]
    expert_count = router.shape[1]
    picked = chosen[:, :, None] == jnp.arange(expert_count, dtype=jnp.int32)[None, None, :]
    weights = jnp.sum(jnp.where(picked, gate_probs[:, None, :], 0.0), axis=-1)
    assign_count = tok_count * top_count
    flat_pick = picked.reshape(assign_count, expert_count).astype(jnp.int32)
    slot_index = jnp.sum((jnp.cumsum(flat_pick, axis=0) - flat_pick) * flat_pick, axis=-1)
    capacity = 3 * tok_count * top_count // (2 * expert_count)
    target = chosen.reshape(-1) * capacity + slot_index
    expert_in = mixed_in.astype(jnp.bfloat16)
    empty_rows = jnp.zeros((expert_count * capacity, model_width), jnp.bfloat16)
    sending = (
        empty_rows.at[target]
        .set(jnp.repeat(expert_in, top_count, axis=0))
        .reshape(expert_count, capacity, model_width)
    )
    arrived = lax.all_to_all(
        sending, ("context", "expert"), split_axis=0, concat_axis=0, tiled=True
    )
    in_shape = arrived.shape
    row_block = arrived.reshape(-1, model_width)
    gate_pre = jnp.dot(row_block, w_gate[0], preferred_element_type=jnp.float32)
    up_pre = jnp.dot(row_block, w_up[0], preferred_element_type=jnp.float32)
    hidden = (jax.nn.silu(gate_pre) * up_pre).astype(jnp.bfloat16)
    result = (
        jnp.dot(hidden, w_down[0], preferred_element_type=jnp.float32)
        .astype(jnp.bfloat16)
        .reshape(in_shape)
    )
    dispatched = lax.all_to_all(
        result, ("context", "expert"), split_axis=0, concat_axis=0, tiled=True
    )
    expert_out = dispatched.reshape(expert_count * capacity, model_width)[target].reshape(
        tok_count, top_count, model_width
    )
    hidden_out = resid + jnp.sum(weights[:, :, None] * expert_out, axis=1)
    upstream = grad_out[0]
    d_weights = jnp.sum(expert_out * upstream[:, None, :], axis=-1)
    grad_outb = (weights[:, :, None] * upstream[:, None, :]).astype(jnp.bfloat16)
    grad_sending = (
        empty_rows.at[target]
        .set(grad_outb.reshape(assign_count, model_width))
        .reshape(expert_count, capacity, model_width)
    )
    grad_arrived, arrived_all = (
        lax.all_to_all(
            grad_sending, ("context", "expert"), split_axis=0, concat_axis=0, tiled=True
        ),
        lax.all_to_all(sending, ("context", "expert"), split_axis=0, concat_axis=0, tiled=True),
    )
    row_block = arrived_all.reshape(-1, model_width)
    grad_block = grad_arrived.reshape(-1, model_width)
    gate_pre = jnp.dot(row_block, w_gate[0], preferred_element_type=jnp.float32)
    up_pre = jnp.dot(row_block, w_up[0], preferred_element_type=jnp.float32)
    sigmoid_g = jax.nn.sigmoid(gate_pre)
    activated = gate_pre * sigmoid_g
    hidden = (activated * up_pre).astype(jnp.bfloat16)
    grad_hidden = contract(grad_block, w_down[0], 1, 1)
    down_grad = contract(hidden, grad_block, 0, 0)
    grad_gate = (grad_hidden * up_pre * sigmoid_g * (1.0 + gate_pre * (1.0 - sigmoid_g))).astype(
        jnp.bfloat16
    )
    grad_up = (grad_hidden * activated).astype(jnp.bfloat16)
    gate_grad = contract(row_block, grad_gate, 0, 0)
    up_grad = contract(row_block, grad_up, 0, 0)
    grad_rows = (contract(grad_gate, w_gate[0], 1, 1) + contract(grad_up, w_up[0], 1, 1)).astype(
        jnp.bfloat16
    )
    grad_back = lax.all_to_all(
        grad_rows.reshape(grad_arrived.shape),
        ("context", "expert"),
        split_axis=0,
        concat_axis=0,
        tiled=True,
    )
    grad_expert_in = grad_back.reshape(expert_count * capacity, model_width)[target].reshape(
        tok_count, top_count, model_width
    )
    mixed_grad_experts = jnp.sum(grad_expert_in.astype(jnp.float32), axis=1)
    gate_sum, up_sum, down_sum = (
        lax.psum_scatter(
            gate_grad[None].astype(jnp.bfloat16), "dp", scatter_dimension=1, tiled=True
        ).astype(jnp.float32),
        lax.psum_scatter(
            up_grad[None].astype(jnp.bfloat16), "dp", scatter_dimension=1, tiled=True
        ).astype(jnp.float32),
        lax.psum_scatter(
            down_grad[None].astype(jnp.bfloat16), "dp", scatter_dimension=1, tiled=True
        ).astype(jnp.float32),
    )
    d_gates = jnp.sum(jnp.where(picked, d_weights[:, :, None], 0.0), axis=1)
    d_logits = gate_probs * (d_gates - jnp.sum(gate_probs * d_gates, axis=-1, keepdims=True))
    router_part = lax.dot_general(
        mixed_in,
        d_logits,
        (((0,), (0,)), ((), ())),
        precision=lax.Precision.HIGHEST,
        preferred_element_type=jnp.float32,
    )
    d_mixed = mixed_grad_experts + lax.dot_general(
        d_logits,
        router,
        (((1,), (1,)), ((), ())),
        precision=lax.Precision.HIGHEST,
        preferred_element_type=jnp.float32,
    )
    _, second_pull = jax.vjp(rms_scale, resid, moe_gain)
    resid_part, moe_gain_part = second_pull(d_mixed)
    d_resid = upstream + resid_part
    resid_b = d_resid.astype(jnp.bfloat16)
    grad_gathered = lax.all_gather(resid_b, "expert", axis=0, tiled=True)
    out_grad = contract(attended, grad_gathered, 0, 0)
    d_attended = contract(grad_gathered, w_out, 1, 1).astype(jnp.bfloat16)
    grad_blocks = d_attended.reshape(block_count, block_rows, heads_here, HEAD_DIM)

    def backward_block(totals, members):
        query_blk, grad_blk, place_blk, total_blk = members
        query_top = jnp.max(place_blk)

        def dot_step(kb, acc):

            def dot_live(total):
                key_blk, value_blk, kplace = key_piece(kb)
                scores = masked_scores(query_blk, key_blk, place_blk, kplace, score_scale)
                prob_exact = jnp.exp(scores - total_blk[:, :, None])
                d_probs = jnp.einsum(
                    "qhd,khd->hqk", grad_blk, value_blk, preferred_element_type=jnp.float32
                )
                return total + jnp.sum(prob_exact * d_probs, axis=-1)

            return lax.cond(key_lowest[kb] <= query_top, dot_live, lambda total: total, acc)

        row_dot = lax.fori_loop(
            0, key_count, dot_step, jnp.zeros((heads_here, block_rows), jnp.float32)
        )

        def grad_step(kb, carry):

            def grad_live(state):
                key_acc, value_acc, query_acc = state
                start = kb * block_rows
                key_blk, value_blk, kplace = key_piece(kb)
                scores = masked_scores(query_blk, key_blk, place_blk, kplace, score_scale)
                prob_exact = jnp.exp(scores - total_blk[:, :, None])
                prob_b = prob_exact.astype(jnp.bfloat16)
                d_probs = jnp.einsum(
                    "qhd,khd->hqk", grad_blk, value_blk, preferred_element_type=jnp.float32
                )
                d_scores = (prob_exact * (d_probs - row_dot[..., None]) * score_scale).astype(
                    jnp.bfloat16
                )
                query_acc = query_acc + jnp.einsum(
                    "hqk,khd->qhd", d_scores, key_blk, preferred_element_type=jnp.float32
                )
                key_add = jnp.einsum(
                    "hqk,qhd->khd", d_scores, query_blk, preferred_element_type=jnp.float32
                )
                value_add = jnp.einsum(
                    "hqk,qhd->khd", prob_b, grad_blk, preferred_element_type=jnp.float32
                )
                key_acc = lax.dynamic_update_slice_in_dim(
                    key_acc,
                    lax.dynamic_slice_in_dim(key_acc, start, block_rows, 0) + key_add,
                    start,
                    0,
                )
                value_acc = lax.dynamic_update_slice_in_dim(
                    value_acc,
                    lax.dynamic_slice_in_dim(value_acc, start, block_rows, 0) + value_add,
                    start,
                    0,
                )
                return (key_acc, value_acc, query_acc)

            return lax.cond(key_lowest[kb] <= query_top, grad_live, lambda state: state, carry)

        start_grad = (
            totals[0],
            totals[1],
            jnp.zeros((block_rows, heads_here, HEAD_DIM), jnp.float32),
        )
        key_acc, value_acc, d_query = lax.fori_loop(0, key_count, grad_step, start_grad)
        return ((key_acc, value_acc), d_query)

    zero_heads = jnp.zeros((seq_rows, heads_here, HEAD_DIM), jnp.float32)
    (key_acc, value_acc), d_queries = lax.scan(
        backward_block,
        (zero_heads, zero_heads),
        (query_blocks, grad_blocks, place_blocks, log_totals),
    )
    key_grad, value_grad = (
        lax.psum_scatter(
            key_acc.reshape(seq_rows, feat_width).astype(jnp.bfloat16),
            "context",
            scatter_dimension=0,
            tiled=True,
        ).astype(jnp.float32),
        lax.psum_scatter(
            value_acc.reshape(seq_rows, feat_width).astype(jnp.bfloat16),
            "context",
            scatter_dimension=0,
            tiled=True,
        ).astype(jnp.float32),
    )
    d_rotated = jnp.stack([d_queries.reshape(span_rows, feat_width), key_grad])
    _, prep_pull = jax.vjp(prep_local, projected, qk_gain)
    d_pair, qk_part = prep_pull(d_rotated)
    d_proj = jnp.concatenate([d_pair, value_grad[None]], axis=0).astype(jnp.bfloat16)
    qkv_grad = jnp.einsum("rd,krf->kdf", gathered_in, d_proj, preferred_element_type=jnp.float32)
    piece_rows = d_proj
    d_normed = lax.psum_scatter(
        jnp.einsum("krf,kdf->rd", piece_rows, w_qkv, preferred_element_type=jnp.float32).astype(
            jnp.bfloat16
        ),
        "expert",
        scatter_dimension=0,
        tiled=True,
    ).astype(jnp.float32)
    _, first_pull = jax.vjp(rms_scale, tokens, attn_gain)
    token_part, attn_gain_part = first_pull(d_normed)
    grad_in = d_resid + token_part
    qkv_sum, out_sum, qk_sum = (
        lax.psum(qkv_grad.astype(jnp.bfloat16), ("dp", "context")).astype(jnp.float32),
        lax.psum(out_grad.astype(jnp.bfloat16), ("dp", "context")).astype(jnp.float32),
        lax.psum(qk_part.astype(jnp.bfloat16), ("dp", "context")).astype(jnp.float32),
    )
    attn_sum, moe_sum, router_sum = lax.psum(
        (attn_gain_part, moe_gain_part, router_part), ("dp", "context", "expert")
    )
    return (
        hidden_out[None],
        grad_in[None],
        attn_sum,
        qkv_sum,
        qk_sum,
        out_sum,
        moe_sum,
        router_sum,
        gate_sum,
        up_sum,
        down_sum,
    )


def solution(mesh):
    grouped = mesh.shape["context"] == 4 and mesh.shape["expert"] == 4
    on_device = fast_device if grouped else portable_device
    placed = (
        P("dp", ("context", "expert"), None),
        P(),
        P(None, None, "expert"),
        P(None, "expert"),
        P("expert", None),
        P(),
        P(),
        P(("context", "expert"), None, None),
        P(("context", "expert"), None, None),
        P(("context", "expert"), None, None),
        P("dp", ("context", "expert"), None),
        P("dp", ("context", "expert"), None),
    )
    return jax.shard_map(
        on_device,
        mesh=mesh,
        in_specs=placed,
        out_specs=(
            P("dp", ("context", "expert"), None),
            P("dp", ("context", "expert"), None),
            P(),
            P(None, None, "expert"),
            P(None, "expert"),
            P("expert", None),
            P(),
            P(),
            P(("context", "expert"), "dp", None),
            P(("context", "expert"), "dp", None),
            P(("context", "expert"), "dp", None),
        ),
        check_vma=False,
    )
```

```python
import functools

import jax
import jax.numpy as jnp
from jax import lax
from jax.experimental import pallas as pl
from jax.experimental.pallas import tpu as pltpu
from jax.sharding import PartitionSpec as P

HEAD_DIM = 128


norm_eps = 1e-05
rope_base = 10000.0
masked_score = -1e30


def rms_scale(values, gain_vec):
    return (
        values * lax.rsqrt(jnp.mean(values * values, axis=-1, keepdims=True) + norm_eps) * gain_vec
    )


def folded_positions(row_ids, span_rows, block_total):
    block_id = row_ids // span_rows
    offset = row_ids % span_rows
    half_rows = span_rows // 2
    piece_id = jnp.where(offset < half_rows, block_id, 2 * block_total - 1 - block_id)
    return piece_id * half_rows + offset % half_rows


def qk_prep(pair_qk, gain_vec, places):
    row_total = pair_qk.shape[1]
    per_head = pair_qk.reshape(2, row_total, -1, HEAD_DIM)
    scaled = per_head * lax.rsqrt(jnp.mean(per_head * per_head, axis=-1, keepdims=True) + norm_eps)
    scaled = scaled * gain_vec.reshape(2, 1, -1, HEAD_DIM)
    half_dim = HEAD_DIM // 2
    frequency = rope_base ** (-2.0 * jnp.arange(half_dim, dtype=jnp.float32) / HEAD_DIM)
    angles = places.astype(jnp.float32)[:, None] * frequency[None, :]
    cosine = jnp.cos(angles)[None, :, None, :]
    sine_table = jnp.sin(angles)[None, :, None, :]
    first_half = scaled[..., :half_dim]
    second_half = scaled[..., half_dim:]
    turned = jnp.concatenate(
        [
            first_half * cosine - second_half * sine_table,
            second_half * cosine + first_half * sine_table,
        ],
        axis=-1,
    )
    return turned.reshape(2, row_total, -1)


def masked_scores(queries, key_heads, query_places, key_places, score_scale):
    scores = (
        jnp.einsum("qhd,khd->hqk", queries, key_heads, preferred_element_type=jnp.float32)
        * score_scale
    )
    return jnp.where(key_places[None, None, :] <= query_places[None, :, None], scores, masked_score)


def contract(left, right, left_dim, right_dim):
    return lax.dot_general(
        left, right, (((left_dim,), (right_dim,)), ((), ())), preferred_element_type=jnp.float32
    )


def nt_dot(left, right):
    return lax.dot_general(
        left, right, (((1,), (1,)), ((), ())), preferred_element_type=jnp.float32
    )


def tn_dot(left, right):
    return lax.dot_general(
        left, right, (((0,), (0,)), ((), ())), preferred_element_type=jnp.float32
    )


def nn_dot(left, right):
    return jnp.dot(left, right, preferred_element_type=jnp.float32)


def as_row(column):
    wide = jnp.broadcast_to(column, (column.shape[0], 128))
    return jnp.transpose(wide)[0:1]


def piece_start(piece, blocks, half):
    return jnp.where(
        piece < blocks, piece * 2 * half, (2 * blocks - 1 - piece) * 2 * half + half
    )


def attend_kernel(blocks, half, place_ref, q_ref, k_ref, v_ref, out_ref, lse_ref):
    mine = place_ref[0]
    scale = HEAD_DIM ** (-0.5)
    row_ids = lax.broadcasted_iota(jnp.int32, (half, half), 0)
    col_ids = lax.broadcasted_iota(jnp.int32, (half, half), 1)
    for part in range(2):
        own = mine if part == 0 else 2 * blocks - 1 - mine
        rows = pl.ds(part * half, half)
        queries = q_ref[rows, :]

        def tile(piece):
            start = pl.multiple_of(piece_start(piece, blocks, half), half)
            scores = nt_dot(queries, k_ref[pl.ds(start, half), :]) * scale
            return jnp.exp(scores), v_ref[pl.ds(start, half), :]

        def step(piece, carry):
            total, acc = carry
            prob, value = tile(piece)
            total = total + jnp.sum(prob, axis=-1, keepdims=True)
            return total, acc + nn_dot(prob.astype(jnp.bfloat16), value)

        total, acc = lax.fori_loop(
            0,
            own,
            step,
            (jnp.zeros((half, 1), jnp.float32), jnp.zeros((half, HEAD_DIM), jnp.float32)),
        )
        prob, value = tile(own)
        prob = jnp.where(col_ids <= row_ids, prob, 0.0)
        total = total + jnp.sum(prob, axis=-1, keepdims=True)
        acc = acc + nn_dot(prob.astype(jnp.bfloat16), value)
        out_ref[rows, :] = (acc / total).astype(jnp.bfloat16)
        lse_ref[0, :, pl.ds(part * half, half)] = as_row(jnp.log(total))


def attend(place, queries, keys, values, blocks):
    span, feat = queries.shape
    seq = keys.shape[0]
    heads = feat // HEAD_DIM
    half = span // 2
    head_block = lambda rows: pl.BlockSpec((rows, HEAD_DIM), lambda h: (0, h))
    return pl.pallas_call(
        functools.partial(attend_kernel, blocks, half),
        grid=(heads,),
        in_specs=[
            pl.BlockSpec(memory_space=pltpu.SMEM),
            head_block(span),
            head_block(seq),
            head_block(seq),
        ],
        out_specs=[head_block(span), pl.BlockSpec((1, 1, span), lambda h: (h, 0, 0))],
        out_shape=[
            jax.ShapeDtypeStruct((span, feat), jnp.bfloat16),
            jax.ShapeDtypeStruct((heads, 1, span), jnp.float32),
        ],
        name="attend",
    )(place, queries, keys, values)


def attend_back_kernel(
    blocks, half, place_ref, q_ref, g_ref, o_ref, lse_ref, k_ref, v_ref,
    dq_ref, dk_ref, dv_ref, dk_acc, dv_acc,
):
    mine = place_ref[0]
    scale = HEAD_DIM ** (-0.5)
    key_ids = lax.broadcasted_iota(jnp.int32, (half, half), 0)
    query_ids = lax.broadcasted_iota(jnp.int32, (half, half), 1)
    dk_acc[...] = jnp.zeros_like(dk_acc)
    dv_acc[...] = jnp.zeros_like(dv_acc)
    for part in range(2):
        own = mine if part == 0 else 2 * blocks - 1 - mine
        rows = pl.ds(part * half, half)
        queries = q_ref[rows, :]
        grads = g_ref[rows, :]
        lse = lse_ref[0, :, pl.ds(part * half, half)]
        row_dot = as_row(
            jnp.sum(
                grads.astype(jnp.float32) * o_ref[rows, :].astype(jnp.float32),
                axis=-1,
                keepdims=True,
            )
        )

        def tile(piece, masked, acc):
            start = pl.multiple_of(piece_start(piece, blocks, half), half)
            place = pl.ds(start, half)
            keys = k_ref[place, :]
            prob = jnp.exp(nt_dot(keys, queries) * scale - lse)
            if masked:
                prob = jnp.where(key_ids <= query_ids, prob, 0.0)
            d_prob = nt_dot(v_ref[place, :], grads)
            d_score = (prob * (d_prob - row_dot) * scale).astype(jnp.bfloat16)
            dv_acc[place, :] += nn_dot(prob.astype(jnp.bfloat16), grads)
            dk_acc[place, :] += nn_dot(d_score, queries)
            return acc + tn_dot(d_score, keys)

        acc = lax.fori_loop(
            0,
            own,
            lambda piece, acc: tile(piece, False, acc),
            jnp.zeros((half, HEAD_DIM), jnp.float32),
        )
        dq_ref[rows, :] = tile(own, True, acc)
    dk_ref[...] = dk_acc[...].astype(jnp.bfloat16)
    dv_ref[...] = dv_acc[...].astype(jnp.bfloat16)


def attend_back(place, queries, grads, attended, lse, keys, values, blocks):
    span, feat = queries.shape
    seq = keys.shape[0]
    heads = feat // HEAD_DIM
    half = span // 2
    head_block = lambda rows: pl.BlockSpec((rows, HEAD_DIM), lambda h: (0, h))
    return pl.pallas_call(
        functools.partial(attend_back_kernel, blocks, half),
        grid=(heads,),
        in_specs=[
            pl.BlockSpec(memory_space=pltpu.SMEM),
            head_block(span),
            head_block(span),
            head_block(span),
            pl.BlockSpec((1, 1, span), lambda h: (h, 0, 0)),
            head_block(seq),
            head_block(seq),
        ],
        out_specs=[head_block(span), head_block(seq), head_block(seq)],
        out_shape=[
            jax.ShapeDtypeStruct((span, feat), jnp.float32),
            jax.ShapeDtypeStruct((seq, feat), jnp.bfloat16),
            jax.ShapeDtypeStruct((seq, feat), jnp.bfloat16),
        ],
        scratch_shapes=[pltpu.VMEM((seq, HEAD_DIM), jnp.float32)] * 2,
        name="attend_back",
    )(place, queries, grads, attended, lse, keys, values)


def split_pair(values):
    upper = values.astype(jnp.bfloat16)
    lower = (values - upper.astype(jnp.float32)).astype(jnp.bfloat16)
    return upper, lower


MESH_ID = pl.DeviceIdType.MESH
GROUP = 4
VMEM_BYTES = 64 * 1024 * 1024 - 256 * 1024


class Place:
    def __init__(self):
        self.ctx = lax.axis_index("context")
        self.lev = lax.axis_index("expert")
        self.side = self.ctx + 1 - 2 * (self.ctx % 2)
        self.front = (self.ctx + 2) % GROUP
        self.has_above = self.lev < GROUP - 1
        self.has_below = self.lev > 0

    def side_id(self):
        return {"context": self.side}

    def front_id(self):
        return {"context": self.front}

    def above_id(self):
        return {"expert": jnp.minimum(self.lev + 1, GROUP - 1)}

    def below_id(self):
        return {"expert": jnp.maximum(self.lev - 1, 0)}

    def nearest(self, rank):
        flipped = self.lev >= 2
        near = jnp.where(flipped, GROUP - 1 - self.lev, self.lev)
        level = jnp.where(near == 0, rank, jnp.where(rank < 2, 1 - rank, rank))
        return jnp.where(flipped, GROUP - 1 - level, level)

    def greet(self, plane=True, line=True):
        barrier = pltpu.get_barrier_semaphore()

        def call(target):
            pl.semaphore_signal(barrier, inc=1, device_id=target, device_id_type=MESH_ID)

        if plane:
            call(self.side_id())
            call(self.front_id())
        if line:
            pl.when(self.has_above)(lambda: call(self.above_id()))
            pl.when(self.has_below)(lambda: call(self.below_id()))
        peers = 2 if plane else 0
        if line:
            peers = peers + 1 + jnp.where((self.lev > 0) & (self.lev < GROUP - 1), 1, 0)
        pl.semaphore_wait(barrier, peers)


def remote(src, dst, send_sem, recv_sem, target):
    return pltpu.make_async_remote_copy(
        src_ref=src,
        dst_ref=dst,
        send_sem=send_sem,
        recv_sem=recv_sem,
        device_id=target,
        device_id_type=MESH_ID,
    )


def slot(level, member, tok, start=0, count=None):
    count = tok if count is None else count
    return pl.ds(pl.multiple_of(level * GROUP * tok + member * tok + start, tok // 2), count)


def experts_kernel(
    tok, width, experts,
    x_ref, g_ref, wg_ref, wu_ref, wd_ref,
    xo_ref, go_ref, ho_ref, dgo_ref, duo_ref, dw_ref,
    x_all, g_all, wg, wu, wd, hid, dgate, dup,
    line_send, line_recv, side_send, side_recv, front_send, front_recv,
    part_send, part_recv, w_sem, g_sem, out_sem,
):
    at = Place()
    half = tok // 2
    ff = wg.shape[1]
    chunk = min(256, ff)
    own_expert = at.ctx * GROUP + at.lev
    loads = [
        pltpu.make_async_copy(src, dst, w_sem.at[i])
        for i, (src, dst) in enumerate(((wg_ref, wg), (wu_ref, wu), (wd_ref, wd)))
    ]

    def g_load(level, member):
        column = (
            at.ctx if member == 0 else at.side if member == 1 else at.front if member == 2
            else GROUP - 1 - at.ctx
        )
        start = pl.multiple_of((column * GROUP + level) * tok, tok)
        return pltpu.make_async_copy(
            g_ref.at[pl.ds(start, tok)],
            g_all.at[slot(level, member, tok)],
            g_sem.at[level, member],
        )

    def line_copy(rank, level, up):
        place = x_all.at[slot(level, 0, tok)]
        return remote(
            place, place, line_send.at[0 if up else 1, rank], line_recv.at[level],
            at.above_id() if up else at.below_id(),
        )

    def plane_copy(level, member):
        sems = (side_send, side_recv) if member == 1 else (front_send, front_recv)
        return remote(
            x_all.at[slot(level, 0, tok)], x_all.at[slot(level, member, tok)],
            sems[0].at[level], sems[1].at[level],
            at.side_id() if member == 1 else at.front_id(),
        )

    def part_copy(level, member):
        start = 0 if member == 1 else half
        return remote(
            x_all.at[slot(level, member, tok, start, half)],
            x_all.at[slot(level, 3, tok, start, half)],
            part_send.at[member - 1, level], part_recv.at[member - 1, level],
            at.front_id() if member == 1 else at.side_id(),
        )

    def pass_on(rank, act):
        level = at.nearest(rank)

        @pl.when((level <= at.lev) & at.has_above)
        def _():
            act(line_copy(rank, level, True))

        @pl.when((level >= at.lev) & at.has_below)
        def _():
            act(line_copy(rank, level, False))

        act(plane_copy(level, 1))
        act(plane_copy(level, 2))

    begin = lambda copy: copy.start()
    x_own = pltpu.make_async_copy(x_ref, x_all.at[slot(at.lev, 0, tok)], w_sem.at[3])
    x_own.start()
    at.greet()
    x_own.wait()
    pass_on(0, begin)
    for load in loads:
        load.start()

    def all_g(rank, carry):
        level = at.nearest(rank)
        for member in range(GROUP):
            g_load(level, member).start()
        return carry

    lax.fori_loop(0, GROUP, all_g, 0)
    second = at.nearest(1)
    line_copy(1, second, True).wait_recv()
    pass_on(1, begin)
    for load in loads:
        load.wait()

    def out_copies(rows, step):
        pairs = (
            (x_all.at[rows, pl.ds(0, width)], xo_ref.at[rows]),
            (g_all.at[rows], go_ref.at[rows]),
            (hid.at[rows], ho_ref.at[rows]),
            (dgate.at[rows], dgo_ref.at[rows]),
            (dup.at[rows], duo_ref.at[rows]),
        )
        return [
            pltpu.make_async_copy(src, dst, out_sem.at[i, step])
            for i, (src, dst) in enumerate(pairs)
        ]

    lane = lax.broadcasted_iota(jnp.int32, (2 * tok, 128), 1)

    def compute(level, late):
        for member in range(2):
            pl.when(late == 0)(lambda m=member: g_load(level, m).wait())
            pl.when(late == 1)(lambda m=member: g_load(level, m + 2).wait())
        rows = pl.ds(pl.multiple_of(level * GROUP * tok + late * 2 * tok, 2 * tok), 2 * tok)
        tail = x_all[rows, pl.ds(width, 128)].astype(jnp.float32)
        own = (lane == own_expert) | (lane == own_expert + experts)
        factor = jnp.sum(jnp.where(own, tail, 0.0), axis=1, keepdims=True)

        def column(index, total):
            cols = pl.ds(pl.multiple_of(index * chunk, chunk), chunk)
            feats = x_all[rows, pl.ds(0, width)]
            gate_pre = nn_dot(feats, wg[:, cols])
            up_pre = nn_dot(feats, wu[:, cols])
            back = nt_dot(g_all[rows, :], wd[cols, :])
            sig = 1.0 / (1.0 + jnp.exp(-gate_pre))
            active = gate_pre * sig
            hidden = active * up_pre
            hid[rows, cols] = (factor * hidden).astype(jnp.bfloat16)
            grad = factor * back
            dgate[rows, cols] = (
                grad * up_pre * sig * (1.0 + gate_pre * (1.0 - sig))
            ).astype(jnp.bfloat16)
            dup[rows, cols] = (grad * active).astype(jnp.bfloat16)
            return total + jnp.sum(hidden * back, axis=1, keepdims=True)

        d_weight = lax.fori_loop(
            0, ff // chunk, column, jnp.zeros((2 * tok, 1), jnp.float32)
        )
        upper = d_weight.astype(jnp.bfloat16).astype(jnp.float32)
        lower = d_weight - upper
        dw_ref[rows, :] = jnp.where(
            lane == own_expert, upper, jnp.where(lane == own_expert + experts, lower, 0.0)
        ).astype(jnp.bfloat16)
        for copy in out_copies(rows, level * 2 + late):
            copy.start()

    def step(index, carry):
        rank = index // 2
        late = index % 2

        @pl.when((late == 0) & (rank < GROUP))
        def _():
            level = at.nearest(rank)
            plane_copy(level, 1).wait_recv()
            part_copy(level, 1).start()
            plane_copy(level, 2).wait_recv()
            part_copy(level, 2).start()

            @pl.when(rank < GROUP - 2)
            def _():
                coming = at.nearest(rank + 2)
                line_copy(rank + 2, coming, True).wait_recv()
                pass_on(rank + 2, begin)

        @pl.when((late == 1) & (rank >= 1))
        def _():
            level = at.nearest(rank - 1)
            part_copy(level, 1).wait_recv()
            part_copy(level, 2).wait_recv()

        @pl.when(((late == 0) & (rank < GROUP)) | ((late == 1) & (rank >= 1)))
        def _():
            compute(at.nearest(rank - late), late)

        return carry

    lax.fori_loop(0, 2 * GROUP + 2, step, 0)

    def drain(rank, carry):
        pass_on(rank, lambda copy: copy.wait_send())
        level = at.nearest(rank)
        part_copy(level, 1).wait_send()
        part_copy(level, 2).wait_send()
        for late in range(2):
            rows = pl.ds(pl.multiple_of(level * GROUP * tok + late * 2 * tok, 2 * tok), 2 * tok)
            for copy in out_copies(rows, level * 2 + late):
                copy.wait()
        return carry

    lax.fori_loop(0, GROUP, drain, 0)


def run_experts(sending, all_upstream, w_gate, w_up, w_down):
    tok, wide = sending.shape
    width = all_upstream.shape[1]
    ff = w_gate.shape[1]
    total = GROUP * GROUP * tok
    anywhere = pl.BlockSpec(memory_space=pl.ANY)
    bf16 = jnp.bfloat16
    dma = pltpu.SemaphoreType.DMA
    sent = (GROUP * 2 + 1) * tok * wide * 2
    return pl.pallas_call(
        functools.partial(experts_kernel, tok, width, GROUP * GROUP),
        in_specs=[anywhere] * 5,
        out_specs=[anywhere] * 5 + [pl.BlockSpec(memory_space=pltpu.VMEM)],
        out_shape=[
            jax.ShapeDtypeStruct((total, width), bf16),
            jax.ShapeDtypeStruct((total, width), bf16),
            jax.ShapeDtypeStruct((total, ff), bf16),
            jax.ShapeDtypeStruct((total, ff), bf16),
            jax.ShapeDtypeStruct((total, ff), bf16),
            jax.ShapeDtypeStruct((total, 128), bf16),
        ],
        scratch_shapes=[
            pltpu.VMEM((total, wide), bf16),
            pltpu.VMEM((total, width), bf16),
            pltpu.VMEM((width, ff), bf16),
            pltpu.VMEM((width, ff), bf16),
            pltpu.VMEM((ff, width), bf16),
            pltpu.VMEM((total, ff), bf16),
            pltpu.VMEM((total, ff), bf16),
            pltpu.VMEM((total, ff), bf16),
            dma((2, GROUP)),
            dma((GROUP,)),
            dma((GROUP,)),
            dma((GROUP,)),
            dma((GROUP,)),
            dma((GROUP,)),
            dma((2, GROUP)),
            dma((2, GROUP)),
            dma((4,)),
            dma((GROUP, GROUP)),
            dma((5, 2 * GROUP)),
        ],
        compiler_params=pltpu.CompilerParams(
            collective_id=1, has_side_effects=True, vmem_limit_bytes=VMEM_BYTES
        ),
        cost_estimate=pl.CostEstimate(
            flops=6 * total * width * ff, bytes_accessed=60 << 20, transcendentals=0
        ),
        name="experts",
    )(sending, all_upstream, w_gate, w_up, w_down)


def give_back_kernel(tok, width, terms, tailed, *refs):
    refs = list(refs)
    take = lambda n: [refs.pop(0) for _ in range(n)]
    lhs_in, w_in = take(terms), take(terms)
    tail_ref = take(1)[0] if tailed else None
    out_ref = take(1)[0]
    lhs, weight = take(terms), take(terms)
    (
        mine, part_a, part_b, from_side, from_front, from_above, from_below,
        load_sem, part_send, part_recv, plane_send, plane_recv, line_send, line_recv,
    ) = refs
    at = Place()
    half = tok // 2
    wide = mine.shape[1]
    chunk = 256
    f32 = lambda value: value.astype(jnp.float32)
    loads = [
        pltpu.make_async_copy(src, dst, load_sem.at[i])
        for i, (src, dst) in enumerate(zip(lhs_in + w_in, lhs + weight))
    ]
    for load in loads:
        load.start()
    at.greet()
    for load in loads:
        load.wait()

    def compute(level, late):
        rows = pl.ds(pl.multiple_of(level * GROUP * tok + late * 2 * tok, 2 * tok), 2 * tok)
        if tailed:
            mine[rows, pl.ds(width, 128)] = tail_ref[rows, :]

        def column(index, carry):
            cols = pl.ds(pl.multiple_of(index * chunk, chunk), chunk)
            if terms == 2:
                result = nt_dot(lhs[0][rows, :], weight[0][cols, :]) + nt_dot(
                    lhs[1][rows, :], weight[1][cols, :]
                )
            else:
                result = nn_dot(lhs[0][rows, :], weight[0][:, cols])
            mine[rows, cols] = result.astype(jnp.bfloat16)
            return carry

        lax.fori_loop(0, width // chunk, column, 0)

    def part_copy(level, member):
        start = 0 if member == 2 else half
        target = part_a if member == 2 else part_b
        return remote(
            mine.at[slot(level, 3, tok, start, half)], target.at[level],
            part_send.at[member - 1, level], part_recv.at[member - 1, level],
            at.side_id() if member == 1 else at.front_id(),
        )

    def plane_copy(level, member):
        target = from_side if member == 1 else from_front
        return remote(
            mine.at[slot(level, member, tok)], target.at[level],
            plane_send.at[member - 1, level], plane_recv.at[member - 1, level],
            at.side_id() if member == 1 else at.front_id(),
        )

    def line_copy(level, up):
        target = from_below if up else from_above
        return remote(
            mine.at[slot(level, 0, tok)], target.at[level],
            line_send.at[0 if up else 1, level], line_recv.at[0 if up else 1, level],
            at.above_id() if up else at.below_id(),
        )

    def add_into(place, other):
        mine[place, :] = (f32(mine[place, :]) + f32(other)).astype(jnp.bfloat16)

    def finish(level):
        place = slot(level, 0, tok)
        plane_copy(level, 1).wait_recv()
        plane_copy(level, 2).wait_recv()
        out_ref[...] = f32(mine[place, :]) + f32(from_side[level]) + f32(from_front[level])

        @pl.when((level <= at.lev) & at.has_above)
        def _():
            line_copy(level, False).wait_recv()
            out_ref[...] += f32(from_above[level])

        @pl.when((level >= at.lev) & at.has_below)
        def _():
            line_copy(level, True).wait_recv()
            out_ref[...] += f32(from_below[level])

        @pl.when(level != at.lev)
        def _():
            mine[place, :] = out_ref[...].astype(jnp.bfloat16)

        pl.when(level < at.lev)(lambda: line_copy(level, False).start())
        pl.when(level > at.lev)(lambda: line_copy(level, True).start())

    def step(rank, carry):
        @pl.when(rank < GROUP)
        def _():
            level = at.nearest(GROUP - 1 - rank)
            compute(level, 1)
            part_copy(level, 2).start()
            part_copy(level, 1).start()

        @pl.when(rank >= 1)
        def _():
            finish(at.nearest(GROUP - rank))

        @pl.when(rank < GROUP)
        def _():
            level = at.nearest(GROUP - 1 - rank)
            compute(level, 0)
            part_copy(level, 2).wait_recv()
            add_into(slot(level, 1, tok, 0, half), part_a[level])
            plane_copy(level, 1).start()
            part_copy(level, 1).wait_recv()
            add_into(slot(level, 2, tok, half, half), part_b[level])
            plane_copy(level, 2).start()

        return carry

    lax.fori_loop(0, GROUP + 1, step, 0)

    def drain(level, carry):
        for member in (1, 2):
            part_copy(level, member).wait_send()
            plane_copy(level, member).wait_send()
        pl.when(level < at.lev)(lambda: line_copy(level, False).wait_send())
        pl.when(level > at.lev)(lambda: line_copy(level, True).wait_send())
        return carry

    lax.fori_loop(0, GROUP, drain, 0)


def give_back(lhs, weights, tail, ident, name):
    total, ff = lhs[0].shape
    terms = len(lhs)
    width = weights[0].shape[0] if terms == 2 else weights[0].shape[1]
    tok = total // (GROUP * GROUP)
    wide = width + (0 if tail is None else 128)
    bf16 = jnp.bfloat16
    dma = pltpu.SemaphoreType.DMA
    anywhere = pl.BlockSpec(memory_space=pl.ANY)
    vmem = pl.BlockSpec(memory_space=pltpu.VMEM)
    tails = () if tail is None else (tail,)
    return pl.pallas_call(
        functools.partial(give_back_kernel, tok, width, terms, tail is not None),
        in_specs=[anywhere] * (2 * terms) + [vmem] * len(tails),
        out_specs=vmem,
        out_shape=jax.ShapeDtypeStruct((tok, wide), jnp.float32),
        scratch_shapes=[pltpu.VMEM((total, ff), bf16)] * terms
        + [pltpu.VMEM(w.shape, bf16) for w in weights]
        + [
            pltpu.VMEM((total, wide), bf16),
            pltpu.VMEM((GROUP, tok // 2, wide), bf16),
            pltpu.VMEM((GROUP, tok // 2, wide), bf16),
            pltpu.VMEM((GROUP, tok, wide), bf16),
            pltpu.VMEM((GROUP, tok, wide), bf16),
            pltpu.VMEM((GROUP, tok, wide), bf16),
            pltpu.VMEM((GROUP, tok, wide), bf16),
            dma((2 * terms,)),
            dma((2, GROUP)),
            dma((2, GROUP)),
            dma((2, GROUP)),
            dma((2, GROUP)),
            dma((2, GROUP)),
            dma((2, GROUP)),
        ],
        compiler_params=pltpu.CompilerParams(
            collective_id=ident, has_side_effects=True, vmem_limit_bytes=VMEM_BYTES
        ),
        cost_estimate=pl.CostEstimate(
            flops=2 * terms * total * width * ff, bytes_accessed=20 << 20, transcendentals=0
        ),
        name=name,
    )(*lhs, *weights, *tails)


TOKEN_AXES = ("context", "expert")


def fast_device(
    hidden_in,
    attn_gain,
    w_qkv,
    qk_gain,
    w_out,
    moe_gain,
    router,
    w_gate,
    w_up,
    w_down,
    expert_ids,
    grad_out,
):
    tokens = hidden_in[0].astype(jnp.float32)
    upstream = grad_out[0]
    tok_count, model_width = tokens.shape
    context_size = lax.axis_size("context")
    expert_size = lax.axis_size("expert")
    expert_count = router.shape[1]
    span_rows = tok_count * expert_size
    context_index = lax.axis_index("context")
    place = jnp.full((1,), context_index, jnp.int32)
    local_places = folded_positions(
        context_index * span_rows + jnp.arange(span_rows, dtype=jnp.int32), span_rows, context_size
    )

    normed_b = rms_scale(tokens, attn_gain).astype(jnp.bfloat16)
    gathered_in = lax.all_gather(normed_b, "expert", axis=0, tiled=True)
    all_upstream = lax.all_gather(
        upstream.astype(jnp.bfloat16), TOKEN_AXES, axis=0, tiled=True
    )
    projected = jnp.einsum(
        "rd,kdf->krf", gathered_in, w_qkv[:2], preferred_element_type=jnp.float32
    )
    value_local = nn_dot(gathered_in, w_qkv[2]).astype(jnp.bfloat16)

    def prep_local(pair_qk, gain_vec):
        return qk_prep(pair_qk, gain_vec, local_places)

    rotated = prep_local(projected, qk_gain).astype(jnp.bfloat16)
    feat_width = projected.shape[2]
    keys_all = lax.all_gather(rotated[1], "context", axis=0, tiled=True)
    values_all = lax.all_gather(value_local, "context", axis=0, tiled=True)
    attended, lse = attend(place, rotated[0], keys_all, values_all, context_size)
    branch_out = lax.psum_scatter(
        nn_dot(attended, w_out).astype(jnp.bfloat16), "expert", scatter_dimension=0, tiled=True
    ).astype(jnp.float32)
    resid = tokens + branch_out
    mixed_in = rms_scale(resid, moe_gain)
    logits = jnp.dot(
        mixed_in, router, precision=lax.Precision.HIGHEST, preferred_element_type=jnp.float32
    )
    gate_probs = jax.nn.softmax(logits, axis=-1)
    chosen = expert_ids[0]
    picked = jnp.any(
        chosen[:, :, None] == jnp.arange(expert_count, dtype=jnp.int32)[None, None, :], axis=1
    )
    weights = jnp.where(picked, gate_probs, 0.0)
    expert_in = mixed_in.astype(jnp.bfloat16)
    pad = jnp.zeros((tok_count, 128 - 2 * expert_count), jnp.bfloat16)
    sending = jnp.concatenate([expert_in, *split_pair(weights), pad], axis=1)
    rows, upstream_rows, hidden_w, grad_gate, grad_up, d_pairs = run_experts(
        sending, all_upstream, w_gate[0], w_up[0], w_down[0]
    )
    returned = give_back((grad_gate, grad_up), (w_gate[0], w_up[0]), d_pairs, 2, "give_back")
    hidden_out = resid + give_back((hidden_w,), (w_down[0],), None, 3, "combine")

    def over_sequences(grad):
        return lax.psum_scatter(
            grad.astype(jnp.bfloat16)[None], "dp", scatter_dimension=1, tiled=True
        ).astype(jnp.float32)

    gate_sum = over_sequences(tn_dot(rows, grad_gate))
    up_sum = over_sequences(tn_dot(rows, grad_up))
    down_sum = over_sequences(tn_dot(hidden_w, upstream_rows))

    d_weights = (
        returned[:, model_width : model_width + expert_count]
        + returned[:, model_width + expert_count : model_width + 2 * expert_count]
    )
    d_gates = jnp.where(picked, d_weights, 0.0)
    d_logits = gate_probs * (d_gates - jnp.sum(gate_probs * d_gates, axis=-1, keepdims=True))
    router_part = lax.dot_general(
        mixed_in,
        d_logits,
        (((0,), (0,)), ((), ())),
        precision=lax.Precision.HIGHEST,
        preferred_element_type=jnp.float32,
    )
    d_mixed = returned[:, :model_width] + lax.dot_general(
        d_logits,
        router,
        (((1,), (1,)), ((), ())),
        precision=lax.Precision.HIGHEST,
        preferred_element_type=jnp.float32,
    )
    _, second_pull = jax.vjp(rms_scale, resid, moe_gain)
    resid_part, moe_gain_part = second_pull(d_mixed)
    d_resid = upstream + resid_part
    grad_gathered = lax.all_gather(
        d_resid.astype(jnp.bfloat16), "expert", axis=0, tiled=True
    )
    out_grad = tn_dot(attended, grad_gathered)
    d_attended = nt_dot(grad_gathered, w_out).astype(jnp.bfloat16)
    d_queries, key_part, value_part = attend_back(
        place, rotated[0], d_attended, attended, lse, keys_all, values_all, context_size
    )
    key_grad = lax.psum_scatter(
        key_part, "context", scatter_dimension=0, tiled=True
    ).astype(jnp.float32)
    value_grad = lax.psum_scatter(
        value_part, "context", scatter_dimension=0, tiled=True
    ).astype(jnp.float32)
    d_rotated = jnp.stack([d_queries, key_grad])
    _, prep_pull = jax.vjp(prep_local, projected, qk_gain)
    d_pair, qk_part = prep_pull(d_rotated)
    d_proj = jnp.concatenate([d_pair, value_grad[None]], axis=0).astype(jnp.bfloat16)
    qkv_grad = jnp.einsum("rd,krf->kdf", gathered_in, d_proj, preferred_element_type=jnp.float32)
    d_normed = lax.psum_scatter(
        jnp.einsum("krf,kdf->rd", d_proj, w_qkv, preferred_element_type=jnp.float32).astype(
            jnp.bfloat16
        ),
        "expert",
        scatter_dimension=0,
        tiled=True,
    ).astype(jnp.float32)
    _, first_pull = jax.vjp(rms_scale, tokens, attn_gain)
    token_part, attn_gain_part = first_pull(d_normed)
    grad_in = d_resid + token_part
    qkv_sum, out_sum, qk_sum = (
        lax.psum(qkv_grad.astype(jnp.bfloat16), ("dp", "context")).astype(jnp.float32),
        lax.psum(out_grad.astype(jnp.bfloat16), ("dp", "context")).astype(jnp.float32),
        lax.psum(qk_part.astype(jnp.bfloat16), ("dp", "context")).astype(jnp.float32),
    )
    attn_sum, moe_sum, router_sum = lax.psum(
        (attn_gain_part, moe_gain_part, router_part), ("dp", "context", "expert")
    )
    return (
        hidden_out[None],
        grad_in[None],
        attn_sum,
        qkv_sum,
        qk_sum,
        out_sum,
        moe_sum,
        router_sum,
        gate_sum,
        up_sum,
        down_sum,
    )


def portable_device(
    hidden_in,
    attn_gain,
    w_qkv,
    qk_gain,
    w_out,
    moe_gain,
    router,
    w_gate,
    w_up,
    w_down,
    expert_ids,
    grad_out,
):
    tokens = hidden_in[0].astype(jnp.float32)
    tok_count = tokens.shape[0]
    model_width = tokens.shape[1]
    context_size = lax.axis_size("context")
    expert_size = lax.axis_size("expert")
    span_rows = tok_count * expert_size
    seq_rows = span_rows * context_size
    context_index = lax.axis_index("context")
    local_places = folded_positions(
        context_index * span_rows + jnp.arange(span_rows, dtype=jnp.int32), span_rows, context_size
    )
    key_places = folded_positions(jnp.arange(seq_rows, dtype=jnp.int32), span_rows, context_size)
    score_scale = HEAD_DIM ** (-0.5)
    normed_b = rms_scale(tokens, attn_gain).astype(jnp.bfloat16)
    gathered_in = lax.all_gather(normed_b, "expert", axis=0, tiled=True)
    projected = jnp.einsum(
        "rd,kdf->krf", gathered_in, w_qkv[:2], preferred_element_type=jnp.float32
    )
    value_local = jnp.dot(gathered_in, w_qkv[2], preferred_element_type=jnp.float32).astype(
        jnp.bfloat16
    )
    feat_width = projected.shape[2]
    heads_here = feat_width // HEAD_DIM

    def prep_local(pair_qk, gain_vec):
        return qk_prep(pair_qk, gain_vec, local_places)

    rotated = prep_local(projected, qk_gain).astype(jnp.bfloat16)
    keys_all, values_all = (
        lax.all_gather(rotated[1], "context", axis=0, tiled=True),
        lax.all_gather(value_local, "context", axis=0, tiled=True),
    )
    key_heads = keys_all.reshape(seq_rows, heads_here, HEAD_DIM)
    value_heads = values_all.reshape(seq_rows, heads_here, HEAD_DIM)
    block_rows = min(512, span_rows)
    block_count = span_rows // block_rows
    key_count = seq_rows // block_rows
    key_lowest = jnp.min(key_places.reshape(key_count, block_rows), axis=1)
    query_blocks = rotated[0].reshape(block_count, block_rows, heads_here, HEAD_DIM)
    place_blocks = local_places.reshape(block_count, block_rows)

    def key_piece(kb):
        start = kb * block_rows
        return (
            lax.dynamic_slice_in_dim(key_heads, start, block_rows, 0),
            lax.dynamic_slice_in_dim(value_heads, start, block_rows, 0),
            lax.dynamic_slice_in_dim(key_places, start, block_rows, 0),
        )

    def attend_blocks(members):
        queries, query_places = members
        query_top = jnp.max(query_places)

        def stat_step(kb, carry):

            def stat_live(state):
                run_max, run_sum = state
                key_blk, value_blk, kplace = key_piece(kb)
                scores = masked_scores(queries, key_blk, query_places, kplace, score_scale)
                new_max = jnp.maximum(run_max, jnp.max(scores, axis=-1))
                new_sum = run_sum * jnp.exp(run_max - new_max) + jnp.sum(
                    jnp.exp(scores - new_max[..., None]), axis=-1
                )
                return (new_max, new_sum)

            return lax.cond(key_lowest[kb] <= query_top, stat_live, lambda state: state, carry)

        start_stat = (
            jnp.full((heads_here, block_rows), masked_score, jnp.float32),
            jnp.zeros((heads_here, block_rows), jnp.float32),
        )
        run_max, run_sum = lax.fori_loop(0, key_count, stat_step, start_stat)
        log_total = run_max + jnp.log(run_sum)

        def value_step(kb, acc):

            def value_live(total):
                key_blk, value_blk, kplace = key_piece(kb)
                scores = masked_scores(queries, key_blk, query_places, kplace, score_scale)
                prob_b = jnp.exp(scores - log_total[..., None]).astype(jnp.bfloat16)
                return total + jnp.einsum(
                    "hqk,khd->qhd", prob_b, value_blk, preferred_element_type=jnp.float32
                )

            return lax.cond(key_lowest[kb] <= query_top, value_live, lambda total: total, acc)

        result = lax.fori_loop(
            0, key_count, value_step, jnp.zeros((block_rows, heads_here, HEAD_DIM), jnp.float32)
        )
        return (result.astype(jnp.bfloat16), log_total)

    attended, log_totals = lax.map(attend_blocks, (query_blocks, place_blocks))
    attended = attended.reshape(span_rows, feat_width)
    piece_rows = attended
    branch_out = lax.psum_scatter(
        jnp.dot(piece_rows, w_out, preferred_element_type=jnp.float32).astype(jnp.bfloat16),
        "expert",
        scatter_dimension=0,
        tiled=True,
    ).astype(jnp.float32)
    resid = tokens + branch_out
    mixed_in = rms_scale(resid, moe_gain)
    logits = jnp.dot(
        mixed_in, router, precision=lax.Precision.HIGHEST, preferred_element_type=jnp.float32
    )
    gate_probs = jax.nn.softmax(logits, axis=-1)
    chosen = expert_ids[0]
    top_count = chosen.shape[1]
    expert_count = router.shape[1]
    picked = chosen[:, :, None] == jnp.arange(expert_count, dtype=jnp.int32)[None, None, :]
    weights = jnp.sum(jnp.where(picked, gate_probs[:, None, :], 0.0), axis=-1)
    assign_count = tok_count * top_count
    flat_pick = picked.reshape(assign_count, expert_count).astype(jnp.int32)
    slot_index = jnp.sum((jnp.cumsum(flat_pick, axis=0) - flat_pick) * flat_pick, axis=-1)
    capacity = 3 * tok_count * top_count // (2 * expert_count)
    target = chosen.reshape(-1) * capacity + slot_index
    expert_in = mixed_in.astype(jnp.bfloat16)
    empty_rows = jnp.zeros((expert_count * capacity, model_width), jnp.bfloat16)
    sending = (
        empty_rows.at[target]
        .set(jnp.repeat(expert_in, top_count, axis=0))
        .reshape(expert_count, capacity, model_width)
    )
    arrived = lax.all_to_all(
        sending, ("context", "expert"), split_axis=0, concat_axis=0, tiled=True
    )
    in_shape = arrived.shape
    row_block = arrived.reshape(-1, model_width)
    gate_pre = jnp.dot(row_block, w_gate[0], preferred_element_type=jnp.float32)
    up_pre = jnp.dot(row_block, w_up[0], preferred_element_type=jnp.float32)
    hidden = (jax.nn.silu(gate_pre) * up_pre).astype(jnp.bfloat16)
    result = (
        jnp.dot(hidden, w_down[0], preferred_element_type=jnp.float32)
        .astype(jnp.bfloat16)
        .reshape(in_shape)
    )
    dispatched = lax.all_to_all(
        result, ("context", "expert"), split_axis=0, concat_axis=0, tiled=True
    )
    expert_out = dispatched.reshape(expert_count * capacity, model_width)[target].reshape(
        tok_count, top_count, model_width
    )
    hidden_out = resid + jnp.sum(weights[:, :, None] * expert_out, axis=1)
    upstream = grad_out[0]
    d_weights = jnp.sum(expert_out * upstream[:, None, :], axis=-1)
    grad_outb = (weights[:, :, None] * upstream[:, None, :]).astype(jnp.bfloat16)
    grad_sending = (
        empty_rows.at[target]
        .set(grad_outb.reshape(assign_count, model_width))
        .reshape(expert_count, capacity, model_width)
    )
    grad_arrived, arrived_all = (
        lax.all_to_all(
            grad_sending, ("context", "expert"), split_axis=0, concat_axis=0, tiled=True
        ),
        lax.all_to_all(sending, ("context", "expert"), split_axis=0, concat_axis=0, tiled=True),
    )
    row_block = arrived_all.reshape(-1, model_width)
    grad_block = grad_arrived.reshape(-1, model_width)
    gate_pre = jnp.dot(row_block, w_gate[0], preferred_element_type=jnp.float32)
    up_pre = jnp.dot(row_block, w_up[0], preferred_element_type=jnp.float32)
    sigmoid_g = jax.nn.sigmoid(gate_pre)
    activated = gate_pre * sigmoid_g
    hidden = (activated * up_pre).astype(jnp.bfloat16)
    grad_hidden = contract(grad_block, w_down[0], 1, 1)
    down_grad = contract(hidden, grad_block, 0, 0)
    grad_gate = (grad_hidden * up_pre * sigmoid_g * (1.0 + gate_pre * (1.0 - sigmoid_g))).astype(
        jnp.bfloat16
    )
    grad_up = (grad_hidden * activated).astype(jnp.bfloat16)
    gate_grad = contract(row_block, grad_gate, 0, 0)
    up_grad = contract(row_block, grad_up, 0, 0)
    grad_rows = (contract(grad_gate, w_gate[0], 1, 1) + contract(grad_up, w_up[0], 1, 1)).astype(
        jnp.bfloat16
    )
    grad_back = lax.all_to_all(
        grad_rows.reshape(grad_arrived.shape),
        ("context", "expert"),
        split_axis=0,
        concat_axis=0,
        tiled=True,
    )
    grad_expert_in = grad_back.reshape(expert_count * capacity, model_width)[target].reshape(
        tok_count, top_count, model_width
    )
    mixed_grad_experts = jnp.sum(grad_expert_in.astype(jnp.float32), axis=1)
    gate_sum, up_sum, down_sum = (
        lax.psum_scatter(
            gate_grad[None].astype(jnp.bfloat16), "dp", scatter_dimension=1, tiled=True
        ).astype(jnp.float32),
        lax.psum_scatter(
            up_grad[None].astype(jnp.bfloat16), "dp", scatter_dimension=1, tiled=True
        ).astype(jnp.float32),
        lax.psum_scatter(
            down_grad[None].astype(jnp.bfloat16), "dp", scatter_dimension=1, tiled=True
        ).astype(jnp.float32),
    )
    d_gates = jnp.sum(jnp.where(picked, d_weights[:, :, None], 0.0), axis=1)
    d_logits = gate_probs * (d_gates - jnp.sum(gate_probs * d_gates, axis=-1, keepdims=True))
    router_part = lax.dot_general(
        mixed_in,
        d_logits,
        (((0,), (0,)), ((), ())),
        precision=lax.Precision.HIGHEST,
        preferred_element_type=jnp.float32,
    )
    d_mixed = mixed_grad_experts + lax.dot_general(
        d_logits,
        router,
        (((1,), (1,)), ((), ())),
        precision=lax.Precision.HIGHEST,
        preferred_element_type=jnp.float32,
    )
    _, second_pull = jax.vjp(rms_scale, resid, moe_gain)
    resid_part, moe_gain_part = second_pull(d_mixed)
    d_resid = upstream + resid_part
    resid_b = d_resid.astype(jnp.bfloat16)
    grad_gathered = lax.all_gather(resid_b, "expert", axis=0, tiled=True)
    out_grad = contract(attended, grad_gathered, 0, 0)
    d_attended = contract(grad_gathered, w_out, 1, 1).astype(jnp.bfloat16)
    grad_blocks = d_attended.reshape(block_count, block_rows, heads_here, HEAD_DIM)

    def backward_block(totals, members):
        query_blk, grad_blk, place_blk, total_blk = members
        query_top = jnp.max(place_blk)

        def dot_step(kb, acc):

            def dot_live(total):
                key_blk, value_blk, kplace = key_piece(kb)
                scores = masked_scores(query_blk, key_blk, place_blk, kplace, score_scale)
                prob_exact = jnp.exp(scores - total_blk[:, :, None])
                d_probs = jnp.einsum(
                    "qhd,khd->hqk", grad_blk, value_blk, preferred_element_type=jnp.float32
                )
                return total + jnp.sum(prob_exact * d_probs, axis=-1)

            return lax.cond(key_lowest[kb] <= query_top, dot_live, lambda total: total, acc)

        row_dot = lax.fori_loop(
            0, key_count, dot_step, jnp.zeros((heads_here, block_rows), jnp.float32)
        )

        def grad_step(kb, carry):

            def grad_live(state):
                key_acc, value_acc, query_acc = state
                start = kb * block_rows
                key_blk, value_blk, kplace = key_piece(kb)
                scores = masked_scores(query_blk, key_blk, place_blk, kplace, score_scale)
                prob_exact = jnp.exp(scores - total_blk[:, :, None])
                prob_b = prob_exact.astype(jnp.bfloat16)
                d_probs = jnp.einsum(
                    "qhd,khd->hqk", grad_blk, value_blk, preferred_element_type=jnp.float32
                )
                d_scores = (prob_exact * (d_probs - row_dot[..., None]) * score_scale).astype(
                    jnp.bfloat16
                )
                query_acc = query_acc + jnp.einsum(
                    "hqk,khd->qhd", d_scores, key_blk, preferred_element_type=jnp.float32
                )
                key_add = jnp.einsum(
                    "hqk,qhd->khd", d_scores, query_blk, preferred_element_type=jnp.float32
                )
                value_add = jnp.einsum(
                    "hqk,qhd->khd", prob_b, grad_blk, preferred_element_type=jnp.float32
                )
                key_acc = lax.dynamic_update_slice_in_dim(
                    key_acc,
                    lax.dynamic_slice_in_dim(key_acc, start, block_rows, 0) + key_add,
                    start,
                    0,
                )
                value_acc = lax.dynamic_update_slice_in_dim(
                    value_acc,
                    lax.dynamic_slice_in_dim(value_acc, start, block_rows, 0) + value_add,
                    start,
                    0,
                )
                return (key_acc, value_acc, query_acc)

            return lax.cond(key_lowest[kb] <= query_top, grad_live, lambda state: state, carry)

        start_grad = (
            totals[0],
            totals[1],
            jnp.zeros((block_rows, heads_here, HEAD_DIM), jnp.float32),
        )
        key_acc, value_acc, d_query = lax.fori_loop(0, key_count, grad_step, start_grad)
        return ((key_acc, value_acc), d_query)

    zero_heads = jnp.zeros((seq_rows, heads_here, HEAD_DIM), jnp.float32)
    (key_acc, value_acc), d_queries = lax.scan(
        backward_block,
        (zero_heads, zero_heads),
        (query_blocks, grad_blocks, place_blocks, log_totals),
    )
    key_grad, value_grad = (
        lax.psum_scatter(
            key_acc.reshape(seq_rows, feat_width).astype(jnp.bfloat16),
            "context",
            scatter_dimension=0,
            tiled=True,
        ).astype(jnp.float32),
        lax.psum_scatter(
            value_acc.reshape(seq_rows, feat_width).astype(jnp.bfloat16),
            "context",
            scatter_dimension=0,
            tiled=True,
        ).astype(jnp.float32),
    )
    d_rotated = jnp.stack([d_queries.reshape(span_rows, feat_width), key_grad])
    _, prep_pull = jax.vjp(prep_local, projected, qk_gain)
    d_pair, qk_part = prep_pull(d_rotated)
    d_proj = jnp.concatenate([d_pair, value_grad[None]], axis=0).astype(jnp.bfloat16)
    qkv_grad = jnp.einsum("rd,krf->kdf", gathered_in, d_proj, preferred_element_type=jnp.float32)
    piece_rows = d_proj
    d_normed = lax.psum_scatter(
        jnp.einsum("krf,kdf->rd", piece_rows, w_qkv, preferred_element_type=jnp.float32).astype(
            jnp.bfloat16
        ),
        "expert",
        scatter_dimension=0,
        tiled=True,
    ).astype(jnp.float32)
    _, first_pull = jax.vjp(rms_scale, tokens, attn_gain)
    token_part, attn_gain_part = first_pull(d_normed)
    grad_in = d_resid + token_part
    qkv_sum, out_sum, qk_sum = (
        lax.psum(qkv_grad.astype(jnp.bfloat16), ("dp", "context")).astype(jnp.float32),
        lax.psum(out_grad.astype(jnp.bfloat16), ("dp", "context")).astype(jnp.float32),
        lax.psum(qk_part.astype(jnp.bfloat16), ("dp", "context")).astype(jnp.float32),
    )
    attn_sum, moe_sum, router_sum = lax.psum(
        (attn_gain_part, moe_gain_part, router_part), ("dp", "context", "expert")
    )
    return (
        hidden_out[None],
        grad_in[None],
        attn_sum,
        qkv_sum,
        qk_sum,
        out_sum,
        moe_sum,
        router_sum,
        gate_sum,
        up_sum,
        down_sum,
    )


def solution(mesh):
    grouped = mesh.shape["context"] == 4 and mesh.shape["expert"] == 4
    on_device = fast_device if grouped else portable_device
    placed = (
        P("dp", ("context", "expert"), None),
        P(),
        P(None, None, "expert"),
        P(None, "expert"),
        P("expert", None),
        P(),
        P(),
        P(("context", "expert"), None, None),
        P(("context", "expert"), None, None),
        P(("context", "expert"), None, None),
        P("dp", ("context", "expert"), None),
        P("dp", ("context", "expert"), None),
    )
    return jax.shard_map(
        on_device,
        mesh=mesh,
        in_specs=placed,
        out_specs=(
            P("dp", ("context", "expert"), None),
            P("dp", ("context", "expert"), None),
            P(),
            P(None, None, "expert"),
            P(None, "expert"),
            P("expert", None),
            P(),
            P(),
            P(("context", "expert"), "dp", None),
            P(("context", "expert"), "dp", None),
            P(("context", "expert"), "dp", None),
        ),
        check_vma=False,
    )
```

```python
import functools

import jax
import jax.numpy as jnp
from jax import lax
from jax.experimental import pallas as pl
from jax.experimental.pallas import tpu as pltpu
from jax.sharding import PartitionSpec as P

HEAD_DIM = 128


norm_eps = 1e-05
rope_base = 10000.0
masked_score = -1e30


def rms_scale(values, gain_vec):
    return (
        values * lax.rsqrt(jnp.mean(values * values, axis=-1, keepdims=True) + norm_eps) * gain_vec
    )


def folded_positions(row_ids, span_rows, block_total):
    block_id = row_ids // span_rows
    offset = row_ids % span_rows
    half_rows = span_rows // 2
    piece_id = jnp.where(offset < half_rows, block_id, 2 * block_total - 1 - block_id)
    return piece_id * half_rows + offset % half_rows


def qk_prep(pair_qk, gain_vec, places):
    row_total = pair_qk.shape[1]
    per_head = pair_qk.reshape(2, row_total, -1, HEAD_DIM)
    scaled = per_head * lax.rsqrt(jnp.mean(per_head * per_head, axis=-1, keepdims=True) + norm_eps)
    scaled = scaled * gain_vec.reshape(2, 1, -1, HEAD_DIM)
    half_dim = HEAD_DIM // 2
    frequency = rope_base ** (-2.0 * jnp.arange(half_dim, dtype=jnp.float32) / HEAD_DIM)
    angles = places.astype(jnp.float32)[:, None] * frequency[None, :]
    cosine = jnp.cos(angles)[None, :, None, :]
    sine_table = jnp.sin(angles)[None, :, None, :]
    first_half = scaled[..., :half_dim]
    second_half = scaled[..., half_dim:]
    turned = jnp.concatenate(
        [
            first_half * cosine - second_half * sine_table,
            second_half * cosine + first_half * sine_table,
        ],
        axis=-1,
    )
    return turned.reshape(2, row_total, -1)


def masked_scores(queries, key_heads, query_places, key_places, score_scale):
    scores = (
        jnp.einsum("qhd,khd->hqk", queries, key_heads, preferred_element_type=jnp.float32)
        * score_scale
    )
    return jnp.where(key_places[None, None, :] <= query_places[None, :, None], scores, masked_score)


def contract(left, right, left_dim, right_dim):
    return lax.dot_general(
        left, right, (((left_dim,), (right_dim,)), ((), ())), preferred_element_type=jnp.float32
    )


def nt_dot(left, right):
    return lax.dot_general(
        left, right, (((1,), (1,)), ((), ())), preferred_element_type=jnp.float32
    )


def tn_dot(left, right):
    return lax.dot_general(
        left, right, (((0,), (0,)), ((), ())), preferred_element_type=jnp.float32
    )


def nn_dot(left, right):
    return jnp.dot(left, right, preferred_element_type=jnp.float32)


def as_row(column):
    wide = jnp.broadcast_to(column, (column.shape[0], 128))
    return jnp.transpose(wide)[0:1]


def piece_start(piece, blocks, half):
    return jnp.where(
        piece < blocks, piece * 2 * half, (2 * blocks - 1 - piece) * 2 * half + half
    )


def attend_kernel(blocks, half, place_ref, q_ref, k_ref, v_ref, out_ref, lse_ref):
    mine = place_ref[0]
    scale = HEAD_DIM ** (-0.5)
    row_ids = lax.broadcasted_iota(jnp.int32, (half, half), 0)
    col_ids = lax.broadcasted_iota(jnp.int32, (half, half), 1)
    for part in range(2):
        own = mine if part == 0 else 2 * blocks - 1 - mine
        rows = pl.ds(part * half, half)
        queries = q_ref[rows, :]

        def tile(piece):
            start = pl.multiple_of(piece_start(piece, blocks, half), half)
            scores = nt_dot(queries, k_ref[pl.ds(start, half), :]) * scale
            return jnp.exp(scores), v_ref[pl.ds(start, half), :]

        def step(piece, carry):
            total, acc = carry
            prob, value = tile(piece)
            total = total + jnp.sum(prob, axis=-1, keepdims=True)
            return total, acc + nn_dot(prob.astype(jnp.bfloat16), value)

        total, acc = lax.fori_loop(
            0,
            own,
            step,
            (jnp.zeros((half, 1), jnp.float32), jnp.zeros((half, HEAD_DIM), jnp.float32)),
        )
        prob, value = tile(own)
        prob = jnp.where(col_ids <= row_ids, prob, 0.0)
        total = total + jnp.sum(prob, axis=-1, keepdims=True)
        acc = acc + nn_dot(prob.astype(jnp.bfloat16), value)
        out_ref[rows, :] = (acc / total).astype(jnp.bfloat16)
        lse_ref[0, :, pl.ds(part * half, half)] = as_row(jnp.log(total))


def attend(place, queries, keys, values, blocks):
    span, feat = queries.shape
    seq = keys.shape[0]
    heads = feat // HEAD_DIM
    half = span // 2
    head_block = lambda rows: pl.BlockSpec((rows, HEAD_DIM), lambda h: (0, h))
    return pl.pallas_call(
        functools.partial(attend_kernel, blocks, half),
        grid=(heads,),
        in_specs=[
            pl.BlockSpec(memory_space=pltpu.SMEM),
            head_block(span),
            head_block(seq),
            head_block(seq),
        ],
        out_specs=[head_block(span), pl.BlockSpec((1, 1, span), lambda h: (h, 0, 0))],
        out_shape=[
            jax.ShapeDtypeStruct((span, feat), jnp.bfloat16),
            jax.ShapeDtypeStruct((heads, 1, span), jnp.float32),
        ],
        name="attend",
    )(place, queries, keys, values)


def attend_back_kernel(
    blocks, half, place_ref, q_ref, g_ref, o_ref, lse_ref, k_ref, v_ref,
    dq_ref, dk_ref, dv_ref, dk_acc, dv_acc,
):
    mine = place_ref[0]
    scale = HEAD_DIM ** (-0.5)
    key_ids = lax.broadcasted_iota(jnp.int32, (half, half), 0)
    query_ids = lax.broadcasted_iota(jnp.int32, (half, half), 1)
    dk_acc[...] = jnp.zeros_like(dk_acc)
    dv_acc[...] = jnp.zeros_like(dv_acc)
    for part in range(2):
        own = mine if part == 0 else 2 * blocks - 1 - mine
        rows = pl.ds(part * half, half)
        queries = q_ref[rows, :]
        grads = g_ref[rows, :]
        lse = lse_ref[0, :, pl.ds(part * half, half)]
        row_dot = as_row(
            jnp.sum(
                grads.astype(jnp.float32) * o_ref[rows, :].astype(jnp.float32),
                axis=-1,
                keepdims=True,
            )
        )

        def tile(piece, masked, acc):
            start = pl.multiple_of(piece_start(piece, blocks, half), half)
            place = pl.ds(start, half)
            keys = k_ref[place, :]
            prob = jnp.exp(nt_dot(keys, queries) * scale - lse)
            if masked:
                prob = jnp.where(key_ids <= query_ids, prob, 0.0)
            d_prob = nt_dot(v_ref[place, :], grads)
            d_score = (prob * (d_prob - row_dot) * scale).astype(jnp.bfloat16)
            dv_acc[place, :] += nn_dot(prob.astype(jnp.bfloat16), grads)
            dk_acc[place, :] += nn_dot(d_score, queries)
            return acc + tn_dot(d_score, keys)

        acc = lax.fori_loop(
            0,
            own,
            lambda piece, acc: tile(piece, False, acc),
            jnp.zeros((half, HEAD_DIM), jnp.float32),
        )
        dq_ref[rows, :] = tile(own, True, acc)
    dk_ref[...] = dk_acc[...].astype(jnp.bfloat16)
    dv_ref[...] = dv_acc[...].astype(jnp.bfloat16)


def attend_back(place, queries, grads, attended, lse, keys, values, blocks):
    span, feat = queries.shape
    seq = keys.shape[0]
    heads = feat // HEAD_DIM
    half = span // 2
    head_block = lambda rows: pl.BlockSpec((rows, HEAD_DIM), lambda h: (0, h))
    return pl.pallas_call(
        functools.partial(attend_back_kernel, blocks, half),
        grid=(heads,),
        in_specs=[
            pl.BlockSpec(memory_space=pltpu.SMEM),
            head_block(span),
            head_block(span),
            head_block(span),
            pl.BlockSpec((1, 1, span), lambda h: (h, 0, 0)),
            head_block(seq),
            head_block(seq),
        ],
        out_specs=[head_block(span), head_block(seq), head_block(seq)],
        out_shape=[
            jax.ShapeDtypeStruct((span, feat), jnp.float32),
            jax.ShapeDtypeStruct((seq, feat), jnp.bfloat16),
            jax.ShapeDtypeStruct((seq, feat), jnp.bfloat16),
        ],
        scratch_shapes=[pltpu.VMEM((seq, HEAD_DIM), jnp.float32)] * 2,
        name="attend_back",
    )(place, queries, grads, attended, lse, keys, values)


def split_pair(values):
    upper = values.astype(jnp.bfloat16)
    lower = (values - upper.astype(jnp.float32)).astype(jnp.bfloat16)
    return upper, lower


MESH_ID = pl.DeviceIdType.MESH
GROUP = 4
VMEM_BYTES = 64 * 1024 * 1024 - 256 * 1024


class Place:
    def __init__(self):
        self.ctx = lax.axis_index("context")
        self.lev = lax.axis_index("expert")
        self.side = self.ctx + 1 - 2 * (self.ctx % 2)
        self.front = (self.ctx + 2) % GROUP
        self.has_above = self.lev < GROUP - 1
        self.has_below = self.lev > 0

    def side_id(self):
        return {"context": self.side}

    def front_id(self):
        return {"context": self.front}

    def pair_id(self):
        return {"dp": 1 - lax.axis_index("dp")}

    def above_id(self):
        return {"expert": jnp.minimum(self.lev + 1, GROUP - 1)}

    def below_id(self):
        return {"expert": jnp.maximum(self.lev - 1, 0)}

    def nearest(self, rank):
        flipped = self.lev >= 2
        near = jnp.where(flipped, GROUP - 1 - self.lev, self.lev)
        level = jnp.where(near == 0, rank, jnp.where(rank < 2, 1 - rank, rank))
        return jnp.where(flipped, GROUP - 1 - level, level)

    def greet(self, plane=True, line=True, pair=False):
        barrier = pltpu.get_barrier_semaphore()

        def call(target):
            pl.semaphore_signal(barrier, inc=1, device_id=target, device_id_type=MESH_ID)

        if plane:
            call(self.side_id())
            call(self.front_id())
        if line:
            pl.when(self.has_above)(lambda: call(self.above_id()))
            pl.when(self.has_below)(lambda: call(self.below_id()))
        if pair:
            call(self.pair_id())
        peers = (2 if plane else 0) + (1 if pair else 0)
        if line:
            peers = peers + 1 + jnp.where((self.lev > 0) & (self.lev < GROUP - 1), 1, 0)
        pl.semaphore_wait(barrier, peers)


def remote(src, dst, send_sem, recv_sem, target):
    return pltpu.make_async_remote_copy(
        src_ref=src,
        dst_ref=dst,
        send_sem=send_sem,
        recv_sem=recv_sem,
        device_id=target,
        device_id_type=MESH_ID,
    )


def slot(level, member, tok, start=0, count=None):
    count = tok if count is None else count
    return pl.ds(pl.multiple_of(level * GROUP * tok + member * tok + start, tok // 2), count)


def experts_kernel(
    tok, width, experts,
    x_ref, g_ref, wg_ref, wu_ref, wd_ref,
    xo_ref, go_ref, ho_ref, dgo_ref, duo_ref, dw_ref,
    x_all, g_all, wg, wu, wd, hid, dgate, dup,
    line_send, line_recv, side_send, side_recv, front_send, front_recv,
    part_send, part_recv, w_sem, g_sem, out_sem,
):
    at = Place()
    half = tok // 2
    ff = wg.shape[1]
    chunk = min(256, ff)
    own_expert = at.ctx * GROUP + at.lev
    loads = [
        pltpu.make_async_copy(src, dst, w_sem.at[i])
        for i, (src, dst) in enumerate(((wg_ref, wg), (wu_ref, wu), (wd_ref, wd)))
    ]

    def g_load(level, member):
        column = (
            at.ctx if member == 0 else at.side if member == 1 else at.front if member == 2
            else GROUP - 1 - at.ctx
        )
        start = pl.multiple_of((column * GROUP + level) * tok, tok)
        return pltpu.make_async_copy(
            g_ref.at[pl.ds(start, tok)],
            g_all.at[slot(level, member, tok)],
            g_sem.at[level, member],
        )

    def line_copy(rank, level, up):
        place = x_all.at[slot(level, 0, tok)]
        return remote(
            place, place, line_send.at[0 if up else 1, rank], line_recv.at[level],
            at.above_id() if up else at.below_id(),
        )

    def plane_copy(level, member):
        sems = (side_send, side_recv) if member == 1 else (front_send, front_recv)
        return remote(
            x_all.at[slot(level, 0, tok)], x_all.at[slot(level, member, tok)],
            sems[0].at[level], sems[1].at[level],
            at.side_id() if member == 1 else at.front_id(),
        )

    def part_copy(level, member):
        start = 0 if member == 1 else half
        return remote(
            x_all.at[slot(level, member, tok, start, half)],
            x_all.at[slot(level, 3, tok, start, half)],
            part_send.at[member - 1, level], part_recv.at[member - 1, level],
            at.front_id() if member == 1 else at.side_id(),
        )

    def pass_on(rank, act):
        level = at.nearest(rank)

        @pl.when((level <= at.lev) & at.has_above)
        def _():
            act(line_copy(rank, level, True))

        @pl.when((level >= at.lev) & at.has_below)
        def _():
            act(line_copy(rank, level, False))

        act(plane_copy(level, 1))
        act(plane_copy(level, 2))

    begin = lambda copy: copy.start()
    x_own = pltpu.make_async_copy(x_ref, x_all.at[slot(at.lev, 0, tok)], w_sem.at[3])
    x_own.start()
    at.greet()
    x_own.wait()
    pass_on(0, begin)
    for load in loads:
        load.start()

    def all_g(rank, carry):
        level = at.nearest(rank)
        for member in range(GROUP):
            g_load(level, member).start()
        return carry

    lax.fori_loop(0, GROUP, all_g, 0)
    second = at.nearest(1)
    line_copy(1, second, True).wait_recv()
    pass_on(1, begin)
    for load in loads:
        load.wait()

    def out_copies(rows, step):
        pairs = (
            (x_all.at[rows, pl.ds(0, width)], xo_ref.at[rows]),
            (g_all.at[rows], go_ref.at[rows]),
            (hid.at[rows], ho_ref.at[rows]),
            (dgate.at[rows], dgo_ref.at[rows]),
            (dup.at[rows], duo_ref.at[rows]),
        )
        return [
            pltpu.make_async_copy(src, dst, out_sem.at[i, step])
            for i, (src, dst) in enumerate(pairs)
        ]

    lane = lax.broadcasted_iota(jnp.int32, (2 * tok, 128), 1)

    def compute(level, late):
        for member in range(2):
            pl.when(late == 0)(lambda m=member: g_load(level, m).wait())
            pl.when(late == 1)(lambda m=member: g_load(level, m + 2).wait())
        rows = pl.ds(pl.multiple_of(level * GROUP * tok + late * 2 * tok, 2 * tok), 2 * tok)
        tail = x_all[rows, pl.ds(width, 128)].astype(jnp.float32)
        own = (lane == own_expert) | (lane == own_expert + experts)
        factor = jnp.sum(jnp.where(own, tail, 0.0), axis=1, keepdims=True)

        def column(index, total):
            cols = pl.ds(pl.multiple_of(index * chunk, chunk), chunk)
            feats = x_all[rows, pl.ds(0, width)]
            gate_pre = nn_dot(feats, wg[:, cols])
            up_pre = nn_dot(feats, wu[:, cols])
            back = nt_dot(g_all[rows, :], wd[cols, :])
            sig = 1.0 / (1.0 + jnp.exp(-gate_pre))
            active = gate_pre * sig
            hidden = active * up_pre
            hid[rows, cols] = (factor * hidden).astype(jnp.bfloat16)
            grad = factor * back
            dgate[rows, cols] = (
                grad * up_pre * sig * (1.0 + gate_pre * (1.0 - sig))
            ).astype(jnp.bfloat16)
            dup[rows, cols] = (grad * active).astype(jnp.bfloat16)
            return total + jnp.sum(hidden * back, axis=1, keepdims=True)

        d_weight = lax.fori_loop(
            0, ff // chunk, column, jnp.zeros((2 * tok, 1), jnp.float32)
        )
        upper = d_weight.astype(jnp.bfloat16).astype(jnp.float32)
        lower = d_weight - upper
        dw_ref[rows, :] = jnp.where(
            lane == own_expert, upper, jnp.where(lane == own_expert + experts, lower, 0.0)
        ).astype(jnp.bfloat16)
        for copy in out_copies(rows, level * 2 + late):
            copy.start()

    def step(index, carry):
        rank = index // 2
        late = index % 2

        @pl.when((late == 0) & (rank < GROUP))
        def _():
            level = at.nearest(rank)
            plane_copy(level, 1).wait_recv()
            part_copy(level, 1).start()
            plane_copy(level, 2).wait_recv()
            part_copy(level, 2).start()

            @pl.when(rank < GROUP - 2)
            def _():
                coming = at.nearest(rank + 2)
                line_copy(rank + 2, coming, True).wait_recv()
                pass_on(rank + 2, begin)

        @pl.when((late == 1) & (rank >= 1))
        def _():
            level = at.nearest(rank - 1)
            part_copy(level, 1).wait_recv()
            part_copy(level, 2).wait_recv()

        @pl.when(((late == 0) & (rank < GROUP)) | ((late == 1) & (rank >= 1)))
        def _():
            compute(at.nearest(rank - late), late)

        return carry

    lax.fori_loop(0, 2 * GROUP + 2, step, 0)

    def drain(rank, carry):
        pass_on(rank, lambda copy: copy.wait_send())
        level = at.nearest(rank)
        part_copy(level, 1).wait_send()
        part_copy(level, 2).wait_send()
        for late in range(2):
            rows = pl.ds(pl.multiple_of(level * GROUP * tok + late * 2 * tok, 2 * tok), 2 * tok)
            for copy in out_copies(rows, level * 2 + late):
                copy.wait()
        return carry

    lax.fori_loop(0, GROUP, drain, 0)


def run_experts(sending, all_upstream, w_gate, w_up, w_down):
    tok, wide = sending.shape
    width = all_upstream.shape[1]
    ff = w_gate.shape[1]
    total = GROUP * GROUP * tok
    anywhere = pl.BlockSpec(memory_space=pl.ANY)
    bf16 = jnp.bfloat16
    dma = pltpu.SemaphoreType.DMA
    sent = (GROUP * 2 + 1) * tok * wide * 2
    return pl.pallas_call(
        functools.partial(experts_kernel, tok, width, GROUP * GROUP),
        in_specs=[anywhere] * 5,
        out_specs=[anywhere] * 5 + [pl.BlockSpec(memory_space=pltpu.VMEM)],
        out_shape=[
            jax.ShapeDtypeStruct((total, width), bf16),
            jax.ShapeDtypeStruct((total, width), bf16),
            jax.ShapeDtypeStruct((total, ff), bf16),
            jax.ShapeDtypeStruct((total, ff), bf16),
            jax.ShapeDtypeStruct((total, ff), bf16),
            jax.ShapeDtypeStruct((total, 128), bf16),
        ],
        scratch_shapes=[
            pltpu.VMEM((total, wide), bf16),
            pltpu.VMEM((total, width), bf16),
            pltpu.VMEM((width, ff), bf16),
            pltpu.VMEM((width, ff), bf16),
            pltpu.VMEM((ff, width), bf16),
            pltpu.VMEM((total, ff), bf16),
            pltpu.VMEM((total, ff), bf16),
            pltpu.VMEM((total, ff), bf16),
            dma((2, GROUP)),
            dma((GROUP,)),
            dma((GROUP,)),
            dma((GROUP,)),
            dma((GROUP,)),
            dma((GROUP,)),
            dma((2, GROUP)),
            dma((2, GROUP)),
            dma((4,)),
            dma((GROUP, GROUP)),
            dma((5, 2 * GROUP)),
        ],
        compiler_params=pltpu.CompilerParams(
            collective_id=1, has_side_effects=True, vmem_limit_bytes=VMEM_BYTES
        ),
        cost_estimate=pl.CostEstimate(
            flops=6 * total * width * ff, bytes_accessed=60 << 20, transcendentals=0
        ),
        name="experts",
    )(sending, all_upstream, w_gate, w_up, w_down)


def give_back_kernel(tok, width, terms, tailed, graded, *refs):
    refs = list(refs)
    take = lambda n: [refs.pop(0) for _ in range(n)]
    lhs_in, w_in = take(terms), take(terms)
    tail_ref = take(1)[0] if tailed else None
    grad_in = take(4) if graded else []
    out_ref = take(1)[0]
    grad_out = take(3) if graded else []
    lhs, weight = take(terms), take(terms)
    (
        mine, part_a, part_b, from_side, from_front, from_above, from_below,
        load_sem, part_send, part_recv, plane_send, plane_recv, line_send, line_recv,
    ) = take(14)
    grads = WeightGrads(grad_in, grad_out, lhs[0], refs) if graded else None
    at = Place()
    half = tok // 2
    wide = mine.shape[1]
    chunk = 256
    f32 = lambda value: value.astype(jnp.float32)
    loads = [
        pltpu.make_async_copy(src, dst, load_sem.at[i])
        for i, (src, dst) in enumerate(zip(lhs_in + w_in, lhs + weight))
    ]
    for load in loads:
        load.start()
    if graded:
        grads.begin()
    at.greet(pair=graded)
    for load in loads:
        load.wait()

    def compute(level, late):
        rows = pl.ds(pl.multiple_of(level * GROUP * tok + late * 2 * tok, 2 * tok), 2 * tok)
        if tailed:
            mine[rows, pl.ds(width, 128)] = tail_ref[rows, :]

        def column(index, carry):
            cols = pl.ds(pl.multiple_of(index * chunk, chunk), chunk)
            if terms == 2:
                result = nt_dot(lhs[0][rows, :], weight[0][cols, :]) + nt_dot(
                    lhs[1][rows, :], weight[1][cols, :]
                )
            else:
                result = nn_dot(lhs[0][rows, :], weight[0][:, cols])
            mine[rows, cols] = result.astype(jnp.bfloat16)
            return carry

        lax.fori_loop(0, width // chunk, column, 0)

    def part_copy(level, member):
        start = 0 if member == 2 else half
        target = part_a if member == 2 else part_b
        return remote(
            mine.at[slot(level, 3, tok, start, half)], target.at[level],
            part_send.at[member - 1, level], part_recv.at[member - 1, level],
            at.side_id() if member == 1 else at.front_id(),
        )

    def plane_copy(level, member):
        target = from_side if member == 1 else from_front
        return remote(
            mine.at[slot(level, member, tok)], target.at[level],
            plane_send.at[member - 1, level], plane_recv.at[member - 1, level],
            at.side_id() if member == 1 else at.front_id(),
        )

    def line_copy(level, up):
        target = from_below if up else from_above
        return remote(
            mine.at[slot(level, 0, tok)], target.at[level],
            line_send.at[0 if up else 1, level], line_recv.at[0 if up else 1, level],
            at.above_id() if up else at.below_id(),
        )

    def add_into(place, other):
        mine[place, :] = (f32(mine[place, :]) + f32(other)).astype(jnp.bfloat16)

    def finish(level):
        place = slot(level, 0, tok)
        plane_copy(level, 1).wait_recv()
        plane_copy(level, 2).wait_recv()
        out_ref[...] = f32(mine[place, :]) + f32(from_side[level]) + f32(from_front[level])

        @pl.when((level <= at.lev) & at.has_above)
        def _():
            line_copy(level, False).wait_recv()
            out_ref[...] += f32(from_above[level])

        @pl.when((level >= at.lev) & at.has_below)
        def _():
            line_copy(level, True).wait_recv()
            out_ref[...] += f32(from_below[level])

        @pl.when(level != at.lev)
        def _():
            mine[place, :] = out_ref[...].astype(jnp.bfloat16)

        pl.when(level < at.lev)(lambda: line_copy(level, False).start())
        pl.when(level > at.lev)(lambda: line_copy(level, True).start())

    def step(rank, carry):
        @pl.when(rank < GROUP)
        def _():
            level = at.nearest(GROUP - 1 - rank)
            compute(level, 1)
            part_copy(level, 2).start()
            part_copy(level, 1).start()
            if graded:
                grads.tiles(rank * 3, 2)

        @pl.when(rank >= 1)
        def _():
            finish(at.nearest(GROUP - rank))

        @pl.when(rank < GROUP)
        def _():
            level = at.nearest(GROUP - 1 - rank)
            compute(level, 0)
            part_copy(level, 2).wait_recv()
            add_into(slot(level, 1, tok, 0, half), part_a[level])
            plane_copy(level, 1).start()
            part_copy(level, 1).wait_recv()
            add_into(slot(level, 2, tok, half, half), part_b[level])
            plane_copy(level, 2).start()
            if graded:
                grads.tiles(rank * 3 + 2, 1)

        return carry

    lax.fori_loop(0, GROUP + 1, step, 0)
    if graded:
        grads.end()

    def drain(level, carry):
        for member in (1, 2):
            part_copy(level, member).wait_send()
            plane_copy(level, member).wait_send()
        pl.when(level < at.lev)(lambda: line_copy(level, False).wait_send())
        pl.when(level > at.lev)(lambda: line_copy(level, True).wait_send())
        return carry

    lax.fori_loop(0, GROUP, drain, 0)


class WeightGrads:
    def __init__(self, given, outs, hidden, refs):
        self.feats_in, self.ups_in, self.dgate_in, self.dup_in = given
        self.outs = outs
        self.hidden = hidden
        (
            self.left, self.dgate, self.dup, self.turned, self.sent, self.got, self.stage,
            self.load_sem, self.send_sem, self.recv_sem, self.out_sem,
        ) = refs
        self.pair = lax.axis_index("dp")
        self.size = self.turned.shape[0]
        self.wide = self.dgate.shape[1]

    def loads(self):
        return [
            pltpu.make_async_copy(self.feats_in, self.left, self.load_sem.at[0]),
            pltpu.make_async_copy(self.dgate_in, self.dgate, self.load_sem.at[1]),
            pltpu.make_async_copy(self.dup_in, self.dup, self.load_sem.at[2]),
        ]

    def begin(self):
        for load in self.loads():
            load.start()

    def last_load(self):
        return pltpu.make_async_copy(self.ups_in, self.left, self.load_sem.at[3])

    def send(self, piece, place):
        return remote(
            self.sent.at[place], self.got.at[piece],
            self.send_sem.at[piece], self.recv_sem.at[piece],
            {"dp": 1 - self.pair},
        )

    def puts(self, piece, place):
        rows = pl.ds(pl.multiple_of(piece * self.size, self.size), self.size)
        halves = [
            pltpu.make_async_copy(
                self.stage.at[place, :, pl.ds(i * self.wide, self.wide)],
                self.outs[i].at[rows], self.out_sem.at[i, piece],
            )
            for i in range(2)
        ]
        return halves

    def last_put(self, piece, place):
        rows = pl.ds(pl.multiple_of((piece - 4) * self.size, self.size), self.size)
        return pltpu.make_async_copy(
            self.stage.at[place], self.outs[2].at[rows], self.out_sem.at[2, piece]
        )

    def each_put(self, piece, place, act):
        @pl.when(piece < 4)
        def _():
            for copy in self.puts(piece, place):
                act(copy)

        pl.when(piece >= 4)(lambda: act(self.last_put(piece, place)))

    def tile(self, index):
        late = index >= 8
        inner = index - jnp.where(late, 8, 0)
        count = jnp.where(late, 2, 4)
        own = inner >= count
        local = jnp.where(own, inner - count, inner)
        piece = local + jnp.where(late, 4, 0)
        owner = jnp.where(own, self.pair, 1 - self.pair)
        cols = pl.ds(pl.multiple_of((owner * count + local) * self.size, self.size), self.size)
        place = local % 2
        keep = lambda copy: copy.wait()

        @pl.when(index == 0)
        def _():
            for load in self.loads():
                load.wait()

        @pl.when(index == 8)
        def _():
            self.last_load().start()
            self.last_load().wait()

        pl.when(late)(lambda: self.turn(self.hidden, cols))
        pl.when(jnp.logical_not(late))(lambda: self.turn(self.left, cols))

        pl.when(jnp.logical_not(own) & (piece >= 2))(lambda: self.send(piece - 2, place).wait_send())

        @pl.when(own)
        def _():
            pl.when(piece >= 2)(lambda: self.each_put(piece - 2, place, keep))
            self.send(piece, place).wait_recv()

        def column(step, carry):
            width = 512
            outs = pl.ds(pl.multiple_of(step * width, width), width)
            per = self.wide // width

            def emit(right):
                value = nn_dot(self.turned[...], right)

                @pl.when(own)
                def _():
                    self.stage[place, :, outs] = value + self.got[piece, :, outs].astype(
                        jnp.float32
                    )

                @pl.when(jnp.logical_not(own))
                def _():
                    self.sent[place, :, outs] = value.astype(jnp.bfloat16)

            narrow = pl.ds(pl.multiple_of((step % per) * width, width), width)
            pl.when(late)(lambda: emit(self.left[:, outs]))
            pl.when(jnp.logical_not(late) & (step < per))(lambda: emit(self.dgate[:, narrow]))
            pl.when(jnp.logical_not(late) & (step >= per))(lambda: emit(self.dup[:, narrow]))
            return carry

        lax.fori_loop(0, 2 * self.wide // 512, column, 0)
        pl.when(own)(lambda: self.each_put(piece, place, lambda copy: copy.start()))
        pl.when(jnp.logical_not(own))(lambda: self.send(piece, place).start())

    def turn(self, source, cols):
        self.turned[...] = jnp.transpose(source[:, cols])

    def tiles(self, first, count):
        def one(step, carry):
            self.tile(first + step)
            return carry

        lax.fori_loop(0, count, one, 0)

    def end(self):
        for piece in (4, 5):
            self.send(piece, piece % 2).wait_send()
            self.last_put(piece, piece % 2).wait()


def give_back(lhs, weights, tail, ident, name, graded=()):
    total, ff = lhs[0].shape
    terms = len(lhs)
    width = weights[0].shape[0] if terms == 2 else weights[0].shape[1]
    tok = total // (GROUP * GROUP)
    wide = width + (0 if tail is None else 128)
    bf16 = jnp.bfloat16
    dma = pltpu.SemaphoreType.DMA
    anywhere = pl.BlockSpec(memory_space=pl.ANY)
    vmem = pl.BlockSpec(memory_space=pltpu.VMEM)
    tails = () if tail is None else (tail,)
    grad_shapes, grad_scratch = [], []
    if graded:
        f32 = jnp.float32
        size = ff // 4
        grad_shapes = [
            jax.ShapeDtypeStruct((width // 2, ff), f32),
            jax.ShapeDtypeStruct((width // 2, ff), f32),
            jax.ShapeDtypeStruct((ff // 2, width), f32),
        ]
        grad_scratch = [
            pltpu.VMEM((total, width), bf16),
            pltpu.VMEM((total, ff), bf16),
            pltpu.VMEM((total, ff), bf16),
            pltpu.VMEM((size, total), bf16),
            pltpu.VMEM((2, size, width), bf16),
            pltpu.VMEM((6, size, width), bf16),
            pltpu.VMEM((2, size, width), f32),
            dma((4,)),
            dma((6,)),
            dma((6,)),
            dma((3, 6)),
        ]
    return pl.pallas_call(
        functools.partial(
            give_back_kernel, tok, width, terms, tail is not None, bool(graded)
        ),
        in_specs=[anywhere] * (2 * terms) + [vmem] * len(tails) + [anywhere] * len(graded),
        out_specs=[vmem] + [anywhere] * len(grad_shapes),
        out_shape=[jax.ShapeDtypeStruct((tok, wide), jnp.float32)] + grad_shapes,
        scratch_shapes=[pltpu.VMEM((total, ff), bf16)] * terms
        + [pltpu.VMEM(w.shape, bf16) for w in weights]
        + [
            pltpu.VMEM((total, wide), bf16),
            pltpu.VMEM((GROUP, tok // 2, wide), bf16),
            pltpu.VMEM((GROUP, tok // 2, wide), bf16),
            pltpu.VMEM((GROUP, tok, wide), bf16),
            pltpu.VMEM((GROUP, tok, wide), bf16),
            pltpu.VMEM((GROUP, tok, wide), bf16),
            pltpu.VMEM((GROUP, tok, wide), bf16),
            dma((2 * terms,)),
            dma((2, GROUP)),
            dma((2, GROUP)),
            dma((2, GROUP)),
            dma((2, GROUP)),
            dma((2, GROUP)),
            dma((2, GROUP)),
        ]
        + grad_scratch,
        compiler_params=pltpu.CompilerParams(
            collective_id=ident, has_side_effects=True, vmem_limit_bytes=VMEM_BYTES
        ),
        cost_estimate=pl.CostEstimate(
            flops=2 * terms * total * width * ff, bytes_accessed=20 << 20, transcendentals=0
        ),
        name=name,
    )(*lhs, *weights, *tails, *graded)


def line_gather_kernel(tok, x_ref, out_ref, send_sem, recv_sem):
    at = Place()
    place = lambda level: pl.ds(pl.multiple_of(level * tok, tok), tok)

    def each(rank, level, act):
        source = x_ref if isinstance(rank, int) and rank == 0 else out_ref.at[place(level)]

        def copy(up):
            return remote(
                source, out_ref.at[place(level)],
                send_sem.at[0 if up else 1, rank], recv_sem.at[level],
                at.above_id() if up else at.below_id(),
            )

        pl.when((level <= at.lev) & at.has_above)(lambda: act(copy(True)))
        pl.when((level >= at.lev) & at.has_below)(lambda: act(copy(False)))

    at.greet(plane=False)
    each(0, at.lev, lambda copy: copy.start())
    out_ref[place(at.lev), :] = x_ref[...]

    def step(rank, carry):
        level = at.nearest(rank)
        target = out_ref.at[place(level)]
        remote(target, target, send_sem.at[0, rank], recv_sem.at[level], at.above_id()).wait_recv()
        each(rank, level, lambda copy: copy.start())
        return carry

    lax.fori_loop(1, GROUP, step, 0)
    each(0, at.lev, lambda copy: copy.wait_send())

    def drain(rank, carry):
        each(rank, at.nearest(rank), lambda copy: copy.wait_send())
        return carry

    lax.fori_loop(1, GROUP, drain, 0)


def remote_call(kernel, outs, scratch, ident, name, *args):
    vmem = pl.BlockSpec(memory_space=pltpu.VMEM)
    return pl.pallas_call(
        kernel,
        in_specs=[vmem] * len(args),
        out_specs=[vmem] * len(outs),
        out_shape=outs,
        scratch_shapes=scratch,
        compiler_params=pltpu.CompilerParams(
            collective_id=ident, has_side_effects=True, vmem_limit_bytes=32 << 20
        ),
        cost_estimate=pl.CostEstimate(flops=0, bytes_accessed=100 << 20, transcendentals=0),
        name=name,
    )(*args)


def line_gather(values, ident, name):
    tok, width = values.shape
    dma = pltpu.SemaphoreType.DMA
    return remote_call(
        functools.partial(line_gather_kernel, tok),
        [jax.ShapeDtypeStruct((GROUP * tok, width), values.dtype)],
        [dma((2, GROUP)), dma((GROUP,))],
        ident, name, values,
    )[0]


def line_scatter_kernel(tok, x_ref, out_ref, carry_up, carry_down, above, below, send_sem, recv_sem):
    at = Place()
    place = lambda level: pl.ds(pl.multiple_of(level * tok, tok), tok)

    def copy(level, up):
        return remote(
            (carry_up if up else carry_down).at[level], (below if up else above).at[level],
            send_sem.at[0 if up else 1, level], recv_sem.at[0 if up else 1, level],
            at.above_id() if up else at.below_id(),
        )

    at.greet(plane=False)

    def step(rank, carry):
        level = at.nearest(GROUP - 1 - rank)
        out_ref[...] = x_ref[place(level), :].astype(jnp.float32)

        @pl.when((level <= at.lev) & at.has_above)
        def _():
            copy(level, False).wait_recv()
            out_ref[...] += above[level].astype(jnp.float32)

        @pl.when((level >= at.lev) & at.has_below)
        def _():
            copy(level, True).wait_recv()
            out_ref[...] += below[level].astype(jnp.float32)

        @pl.when(level < at.lev)
        def _():
            carry_down[level] = out_ref[...].astype(jnp.bfloat16)
            copy(level, False).start()

        @pl.when(level > at.lev)
        def _():
            carry_up[level] = out_ref[...].astype(jnp.bfloat16)
            copy(level, True).start()

        return carry

    lax.fori_loop(0, GROUP, step, 0)

    def drain(level, carry):
        pl.when(level < at.lev)(lambda: copy(level, False).wait_send())
        pl.when(level > at.lev)(lambda: copy(level, True).wait_send())
        return carry

    lax.fori_loop(0, GROUP, drain, 0)


def line_scatter(values, ident, name):
    rows, width = values.shape
    tok = rows // GROUP
    dma = pltpu.SemaphoreType.DMA
    return remote_call(
        functools.partial(line_scatter_kernel, tok),
        [jax.ShapeDtypeStruct((tok, width), jnp.float32)],
        [pltpu.VMEM((GROUP, tok, width), jnp.bfloat16)] * 4
        + [dma((2, GROUP)), dma((2, GROUP))],
        ident, name, values,
    )[0]


def plane_gather_kernel(rows, count, *refs):
    xs, outs = refs[:count], refs[count : 2 * count]
    send_sem, recv_sem = refs[2 * count :]
    at = Place()
    half = rows // 2
    place = lambda column, start, size: pl.ds(pl.multiple_of(column * rows + start, half), size)

    def full(i, member):
        return remote(
            xs[i], outs[i].at[place(at.ctx, 0, rows)],
            send_sem.at[i, member], recv_sem.at[i, member],
            at.side_id() if member == 0 else at.front_id(),
        )

    def part(i, member):
        column = at.side if member == 0 else at.front
        source = outs[i].at[place(column, member * half, half)]
        return remote(
            source, source, send_sem.at[i, 2 + member], recv_sem.at[i, 2 + member],
            at.front_id() if member == 0 else at.side_id(),
        )

    at.greet(line=False)
    for i in range(count):
        full(i, 0).start()
        full(i, 1).start()
    for i in range(count):
        outs[i][place(at.ctx, 0, rows), :] = xs[i][...]
    for i in range(count):
        for member in range(2):
            full(i, member).wait_recv()
            part(i, member).start()
    for i in range(count):
        for member in range(2):
            part(i, member).wait_recv()
    for i in range(count):
        for member in range(2):
            full(i, member).wait_send()
            part(i, member).wait_send()


def plane_gather(values, ident, name):
    rows, width = values[0].shape
    count = len(values)
    dma = pltpu.SemaphoreType.DMA
    return remote_call(
        functools.partial(plane_gather_kernel, rows, count),
        [jax.ShapeDtypeStruct((GROUP * rows, width), v.dtype) for v in values],
        [dma((count, 4)), dma((count, 4))],
        ident, name, *values,
    )


def plane_scatter_kernel(rows, count, *refs):
    xs, outs = refs[:count], refs[count : 2 * count]
    added, parts, fulls = refs[2 * count : 5 * count : 3], refs[2 * count + 1 : 5 * count : 3], refs[2 * count + 2 : 5 * count : 3]
    send_sem, recv_sem = refs[5 * count :]
    at = Place()
    half = rows // 2
    place = lambda column, start, size: pl.ds(pl.multiple_of(column * rows + start, half), size)
    columns = (at.side, at.front)
    nears = (at.side_id(), at.front_id())

    def part(i, member):
        return remote(
            xs[i].at[place(GROUP - 1 - at.ctx, (1 - member) * half, half)], parts[i].at[member],
            send_sem.at[i, member], recv_sem.at[i, member], nears[member],
        )

    def plain(i, member):
        start = (1 - member) * half
        return remote(
            xs[i].at[place(columns[member], start, half)], fulls[i].at[member, pl.ds(start, half)],
            send_sem.at[i, 2 + member], recv_sem.at[i, 2 + member], nears[member],
        )

    def summed(i, member):
        start = member * half
        return remote(
            added[i].at[member], fulls[i].at[member, pl.ds(start, half)],
            send_sem.at[i, 4 + member], recv_sem.at[i, 4 + member], nears[member],
        )

    at.greet(line=False)
    for i in range(count):
        for member in range(2):
            part(i, member).start()
        for member in range(2):
            plain(i, member).start()
    for i in range(count):
        for member in range(2):
            part(i, 1 - member).wait_recv()
            own = xs[i][place(columns[member], member * half, half), :]
            added[i][member] = (
                own.astype(jnp.float32) + parts[i][1 - member].astype(jnp.float32)
            ).astype(jnp.bfloat16)
            summed(i, member).start()
    for i in range(count):
        total = xs[i][place(at.ctx, 0, rows), :].astype(jnp.float32)
        for member in range(2):
            plain(i, member).wait_recv()
            summed(i, member).wait_recv()
            total = total + fulls[i][member].astype(jnp.float32)
        outs[i][...] = total
    for i in range(count):
        for member in range(2):
            part(i, member).wait_send()
            plain(i, member).wait_send()
            summed(i, member).wait_send()


def plane_scatter(values, ident, name):
    rows, width = values[0].shape
    rows = rows // GROUP
    count = len(values)
    dma = pltpu.SemaphoreType.DMA
    bf16 = jnp.bfloat16
    return remote_call(
        functools.partial(plane_scatter_kernel, rows, count),
        [jax.ShapeDtypeStruct((rows, width), jnp.float32) for _ in values],
        [
            pltpu.VMEM((2, rows // 2, width), bf16),
            pltpu.VMEM((2, rows // 2, width), bf16),
            pltpu.VMEM((2, rows, width), bf16),
        ]
        * count
        + [dma((count, 6)), dma((count, 6))],
        ident, name, *values,
    )


TOKEN_AXES = ("context", "expert")


def small_sums(router_part, moe_gain_part):
    width, experts = router_part.shape
    packed = jnp.concatenate([jnp.transpose(router_part), moe_gain_part[None]], axis=0)
    total = lax.psum(packed, ("dp", "context", "expert"))
    return jnp.transpose(total[:experts]), total[experts]


def fast_device(
    hidden_in,
    attn_gain,
    w_qkv,
    qk_gain,
    w_out,
    moe_gain,
    router,
    w_gate,
    w_up,
    w_down,
    expert_ids,
    grad_out,
):
    tokens = hidden_in[0].astype(jnp.float32)
    upstream = grad_out[0]
    tok_count, model_width = tokens.shape
    context_size = lax.axis_size("context")
    expert_size = lax.axis_size("expert")
    expert_count = router.shape[1]
    span_rows = tok_count * expert_size
    context_index = lax.axis_index("context")
    place = jnp.full((1,), context_index, jnp.int32)
    local_places = folded_positions(
        context_index * span_rows + jnp.arange(span_rows, dtype=jnp.int32), span_rows, context_size
    )

    normed_b = rms_scale(tokens, attn_gain).astype(jnp.bfloat16)
    gathered_in = line_gather(normed_b, 4, "gather_normed")
    all_upstream = lax.all_gather(
        upstream.astype(jnp.bfloat16), TOKEN_AXES, axis=0, tiled=True
    )
    projected = jnp.einsum(
        "rd,kdf->krf", gathered_in, w_qkv[:2], preferred_element_type=jnp.float32
    )
    value_local = nn_dot(gathered_in, w_qkv[2]).astype(jnp.bfloat16)

    def prep_local(pair_qk, gain_vec):
        return qk_prep(pair_qk, gain_vec, local_places)

    rotated = prep_local(projected, qk_gain).astype(jnp.bfloat16)
    feat_width = projected.shape[2]
    keys_all, values_all = plane_gather((rotated[1], value_local), 5, "gather_keys")
    attended, lse = attend(place, rotated[0], keys_all, values_all, context_size)
    branch_out = line_scatter(nn_dot(attended, w_out).astype(jnp.bfloat16), 6, "sum_heads")
    resid = tokens + branch_out
    mixed_in = rms_scale(resid, moe_gain)
    logits = jnp.dot(
        mixed_in, router, precision=lax.Precision.HIGHEST, preferred_element_type=jnp.float32
    )
    gate_probs = jax.nn.softmax(logits, axis=-1)
    chosen = expert_ids[0]
    picked = jnp.any(
        chosen[:, :, None] == jnp.arange(expert_count, dtype=jnp.int32)[None, None, :], axis=1
    )
    weights = jnp.where(picked, gate_probs, 0.0)
    expert_in = mixed_in.astype(jnp.bfloat16)
    pad = jnp.zeros((tok_count, 128 - 2 * expert_count), jnp.bfloat16)
    sending = jnp.concatenate([expert_in, *split_pair(weights), pad], axis=1)
    rows, upstream_rows, hidden_w, grad_gate, grad_up, d_pairs = run_experts(
        sending, all_upstream, w_gate[0], w_up[0], w_down[0]
    )
    returned = give_back((grad_gate, grad_up), (w_gate[0], w_up[0]), d_pairs, 2, "give_back")[0]
    d_weights = (
        returned[:, model_width : model_width + expert_count]
        + returned[:, model_width + expert_count : model_width + 2 * expert_count]
    )
    d_gates = jnp.where(picked, d_weights, 0.0)
    d_logits = gate_probs * (d_gates - jnp.sum(gate_probs * d_gates, axis=-1, keepdims=True))
    router_part = lax.dot_general(
        mixed_in,
        d_logits,
        (((0,), (0,)), ((), ())),
        precision=lax.Precision.HIGHEST,
        preferred_element_type=jnp.float32,
    )
    d_mixed = returned[:, :model_width] + lax.dot_general(
        d_logits,
        router,
        (((1,), (1,)), ((), ())),
        precision=lax.Precision.HIGHEST,
        preferred_element_type=jnp.float32,
    )
    _, second_pull = jax.vjp(rms_scale, resid, moe_gain)
    resid_part, moe_gain_part = second_pull(d_mixed)
    d_resid = upstream + resid_part
    router_sum, moe_sum = small_sums(router_part, moe_gain_part)
    grad_gathered = line_gather(d_resid.astype(jnp.bfloat16), 7, "gather_resid")
    out_grad = tn_dot(attended, grad_gathered)
    d_attended = nt_dot(grad_gathered, w_out).astype(jnp.bfloat16)
    d_queries, key_part, value_part = attend_back(
        place, rotated[0], d_attended, attended, lse, keys_all, values_all, context_size
    )
    key_grad, value_grad = plane_scatter((key_part, value_part), 8, "sum_keys")
    d_rotated = jnp.stack([d_queries, key_grad])
    _, prep_pull = jax.vjp(prep_local, projected, qk_gain)
    d_pair, qk_part = prep_pull(d_rotated)
    d_proj = jnp.concatenate([d_pair, value_grad[None]], axis=0).astype(jnp.bfloat16)
    qkv_grad = jnp.einsum("rd,krf->kdf", gathered_in, d_proj, preferred_element_type=jnp.float32)
    d_normed = line_scatter(
        jnp.einsum("krf,kdf->rd", d_proj, w_qkv, preferred_element_type=jnp.float32).astype(
            jnp.bfloat16
        ),
        9,
        "sum_normed",
    )
    _, first_pull = jax.vjp(rms_scale, tokens, attn_gain)
    token_part, attn_gain_part = first_pull(d_normed)
    grad_in = d_resid + token_part
    combined, gate_sum, up_sum, down_sum = give_back(
        (hidden_w,), (w_down[0],), None, 3, "combine",
        graded=(rows, upstream_rows, grad_gate, grad_up),
    )
    hidden_out = resid + combined
    qkv_sum, out_sum = (
        lax.psum(qkv_grad.astype(jnp.bfloat16), ("dp", "context")).astype(jnp.float32),
        lax.psum(out_grad.astype(jnp.bfloat16), ("dp", "context")).astype(jnp.float32),
    )
    qk_slots = jnp.where(
        jnp.arange(expert_size)[:, None] == lax.axis_index("expert"), qk_part.reshape(1, -1), 0.0
    )
    last = lax.psum(
        jnp.concatenate([attn_gain_part, qk_slots.reshape(-1)]), ("dp", "context", "expert")
    )
    attn_sum = last[:model_width]
    qk_sum = lax.dynamic_index_in_dim(
        last[model_width:].reshape(expert_size, -1), lax.axis_index("expert"), 0, keepdims=False
    ).reshape(qk_part.shape)
    return (
        hidden_out[None],
        grad_in[None],
        attn_sum,
        qkv_sum,
        qk_sum,
        out_sum,
        moe_sum,
        router_sum,
        gate_sum[None],
        up_sum[None],
        down_sum[None],
    )


def portable_device(
    hidden_in,
    attn_gain,
    w_qkv,
    qk_gain,
    w_out,
    moe_gain,
    router,
    w_gate,
    w_up,
    w_down,
    expert_ids,
    grad_out,
):
    tokens = hidden_in[0].astype(jnp.float32)
    tok_count = tokens.shape[0]
    model_width = tokens.shape[1]
    context_size = lax.axis_size("context")
    expert_size = lax.axis_size("expert")
    span_rows = tok_count * expert_size
    seq_rows = span_rows * context_size
    context_index = lax.axis_index("context")
    local_places = folded_positions(
        context_index * span_rows + jnp.arange(span_rows, dtype=jnp.int32), span_rows, context_size
    )
    key_places = folded_positions(jnp.arange(seq_rows, dtype=jnp.int32), span_rows, context_size)
    score_scale = HEAD_DIM ** (-0.5)
    normed_b = rms_scale(tokens, attn_gain).astype(jnp.bfloat16)
    gathered_in = lax.all_gather(normed_b, "expert", axis=0, tiled=True)
    projected = jnp.einsum(
        "rd,kdf->krf", gathered_in, w_qkv[:2], preferred_element_type=jnp.float32
    )
    value_local = jnp.dot(gathered_in, w_qkv[2], preferred_element_type=jnp.float32).astype(
        jnp.bfloat16
    )
    feat_width = projected.shape[2]
    heads_here = feat_width // HEAD_DIM

    def prep_local(pair_qk, gain_vec):
        return qk_prep(pair_qk, gain_vec, local_places)

    rotated = prep_local(projected, qk_gain).astype(jnp.bfloat16)
    keys_all, values_all = (
        lax.all_gather(rotated[1], "context", axis=0, tiled=True),
        lax.all_gather(value_local, "context", axis=0, tiled=True),
    )
    key_heads = keys_all.reshape(seq_rows, heads_here, HEAD_DIM)
    value_heads = values_all.reshape(seq_rows, heads_here, HEAD_DIM)
    block_rows = min(512, span_rows)
    block_count = span_rows // block_rows
    key_count = seq_rows // block_rows
    key_lowest = jnp.min(key_places.reshape(key_count, block_rows), axis=1)
    query_blocks = rotated[0].reshape(block_count, block_rows, heads_here, HEAD_DIM)
    place_blocks = local_places.reshape(block_count, block_rows)

    def key_piece(kb):
        start = kb * block_rows
        return (
            lax.dynamic_slice_in_dim(key_heads, start, block_rows, 0),
            lax.dynamic_slice_in_dim(value_heads, start, block_rows, 0),
            lax.dynamic_slice_in_dim(key_places, start, block_rows, 0),
        )

    def attend_blocks(members):
        queries, query_places = members
        query_top = jnp.max(query_places)

        def stat_step(kb, carry):

            def stat_live(state):
                run_max, run_sum = state
                key_blk, value_blk, kplace = key_piece(kb)
                scores = masked_scores(queries, key_blk, query_places, kplace, score_scale)
                new_max = jnp.maximum(run_max, jnp.max(scores, axis=-1))
                new_sum = run_sum * jnp.exp(run_max - new_max) + jnp.sum(
                    jnp.exp(scores - new_max[..., None]), axis=-1
                )
                return (new_max, new_sum)

            return lax.cond(key_lowest[kb] <= query_top, stat_live, lambda state: state, carry)

        start_stat = (
            jnp.full((heads_here, block_rows), masked_score, jnp.float32),
            jnp.zeros((heads_here, block_rows), jnp.float32),
        )
        run_max, run_sum = lax.fori_loop(0, key_count, stat_step, start_stat)
        log_total = run_max + jnp.log(run_sum)

        def value_step(kb, acc):

            def value_live(total):
                key_blk, value_blk, kplace = key_piece(kb)
                scores = masked_scores(queries, key_blk, query_places, kplace, score_scale)
                prob_b = jnp.exp(scores - log_total[..., None]).astype(jnp.bfloat16)
                return total + jnp.einsum(
                    "hqk,khd->qhd", prob_b, value_blk, preferred_element_type=jnp.float32
                )

            return lax.cond(key_lowest[kb] <= query_top, value_live, lambda total: total, acc)

        result = lax.fori_loop(
            0, key_count, value_step, jnp.zeros((block_rows, heads_here, HEAD_DIM), jnp.float32)
        )
        return (result.astype(jnp.bfloat16), log_total)

    attended, log_totals = lax.map(attend_blocks, (query_blocks, place_blocks))
    attended = attended.reshape(span_rows, feat_width)
    piece_rows = attended
    branch_out = lax.psum_scatter(
        jnp.dot(piece_rows, w_out, preferred_element_type=jnp.float32).astype(jnp.bfloat16),
        "expert",
        scatter_dimension=0,
        tiled=True,
    ).astype(jnp.float32)
    resid = tokens + branch_out
    mixed_in = rms_scale(resid, moe_gain)
    logits = jnp.dot(
        mixed_in, router, precision=lax.Precision.HIGHEST, preferred_element_type=jnp.float32
    )
    gate_probs = jax.nn.softmax(logits, axis=-1)
    chosen = expert_ids[0]
    top_count = chosen.shape[1]
    expert_count = router.shape[1]
    picked = chosen[:, :, None] == jnp.arange(expert_count, dtype=jnp.int32)[None, None, :]
    weights = jnp.sum(jnp.where(picked, gate_probs[:, None, :], 0.0), axis=-1)
    assign_count = tok_count * top_count
    flat_pick = picked.reshape(assign_count, expert_count).astype(jnp.int32)
    slot_index = jnp.sum((jnp.cumsum(flat_pick, axis=0) - flat_pick) * flat_pick, axis=-1)
    capacity = 3 * tok_count * top_count // (2 * expert_count)
    target = chosen.reshape(-1) * capacity + slot_index
    expert_in = mixed_in.astype(jnp.bfloat16)
    empty_rows = jnp.zeros((expert_count * capacity, model_width), jnp.bfloat16)
    sending = (
        empty_rows.at[target]
        .set(jnp.repeat(expert_in, top_count, axis=0))
        .reshape(expert_count, capacity, model_width)
    )
    arrived = lax.all_to_all(
        sending, ("context", "expert"), split_axis=0, concat_axis=0, tiled=True
    )
    in_shape = arrived.shape
    row_block = arrived.reshape(-1, model_width)
    gate_pre = jnp.dot(row_block, w_gate[0], preferred_element_type=jnp.float32)
    up_pre = jnp.dot(row_block, w_up[0], preferred_element_type=jnp.float32)
    hidden = (jax.nn.silu(gate_pre) * up_pre).astype(jnp.bfloat16)
    result = (
        jnp.dot(hidden, w_down[0], preferred_element_type=jnp.float32)
        .astype(jnp.bfloat16)
        .reshape(in_shape)
    )
    dispatched = lax.all_to_all(
        result, ("context", "expert"), split_axis=0, concat_axis=0, tiled=True
    )
    expert_out = dispatched.reshape(expert_count * capacity, model_width)[target].reshape(
        tok_count, top_count, model_width
    )
    hidden_out = resid + jnp.sum(weights[:, :, None] * expert_out, axis=1)
    upstream = grad_out[0]
    d_weights = jnp.sum(expert_out * upstream[:, None, :], axis=-1)
    grad_outb = (weights[:, :, None] * upstream[:, None, :]).astype(jnp.bfloat16)
    grad_sending = (
        empty_rows.at[target]
        .set(grad_outb.reshape(assign_count, model_width))
        .reshape(expert_count, capacity, model_width)
    )
    grad_arrived, arrived_all = (
        lax.all_to_all(
            grad_sending, ("context", "expert"), split_axis=0, concat_axis=0, tiled=True
        ),
        lax.all_to_all(sending, ("context", "expert"), split_axis=0, concat_axis=0, tiled=True),
    )
    row_block = arrived_all.reshape(-1, model_width)
    grad_block = grad_arrived.reshape(-1, model_width)
    gate_pre = jnp.dot(row_block, w_gate[0], preferred_element_type=jnp.float32)
    up_pre = jnp.dot(row_block, w_up[0], preferred_element_type=jnp.float32)
    sigmoid_g = jax.nn.sigmoid(gate_pre)
    activated = gate_pre * sigmoid_g
    hidden = (activated * up_pre).astype(jnp.bfloat16)
    grad_hidden = contract(grad_block, w_down[0], 1, 1)
    down_grad = contract(hidden, grad_block, 0, 0)
    grad_gate = (grad_hidden * up_pre * sigmoid_g * (1.0 + gate_pre * (1.0 - sigmoid_g))).astype(
        jnp.bfloat16
    )
    grad_up = (grad_hidden * activated).astype(jnp.bfloat16)
    gate_grad = contract(row_block, grad_gate, 0, 0)
    up_grad = contract(row_block, grad_up, 0, 0)
    grad_rows = (contract(grad_gate, w_gate[0], 1, 1) + contract(grad_up, w_up[0], 1, 1)).astype(
        jnp.bfloat16
    )
    grad_back = lax.all_to_all(
        grad_rows.reshape(grad_arrived.shape),
        ("context", "expert"),
        split_axis=0,
        concat_axis=0,
        tiled=True,
    )
    grad_expert_in = grad_back.reshape(expert_count * capacity, model_width)[target].reshape(
        tok_count, top_count, model_width
    )
    mixed_grad_experts = jnp.sum(grad_expert_in.astype(jnp.float32), axis=1)
    gate_sum, up_sum, down_sum = (
        lax.psum_scatter(
            gate_grad[None].astype(jnp.bfloat16), "dp", scatter_dimension=1, tiled=True
        ).astype(jnp.float32),
        lax.psum_scatter(
            up_grad[None].astype(jnp.bfloat16), "dp", scatter_dimension=1, tiled=True
        ).astype(jnp.float32),
        lax.psum_scatter(
            down_grad[None].astype(jnp.bfloat16), "dp", scatter_dimension=1, tiled=True
        ).astype(jnp.float32),
    )
    d_gates = jnp.sum(jnp.where(picked, d_weights[:, :, None], 0.0), axis=1)
    d_logits = gate_probs * (d_gates - jnp.sum(gate_probs * d_gates, axis=-1, keepdims=True))
    router_part = lax.dot_general(
        mixed_in,
        d_logits,
        (((0,), (0,)), ((), ())),
        precision=lax.Precision.HIGHEST,
        preferred_element_type=jnp.float32,
    )
    d_mixed = mixed_grad_experts + lax.dot_general(
        d_logits,
        router,
        (((1,), (1,)), ((), ())),
        precision=lax.Precision.HIGHEST,
        preferred_element_type=jnp.float32,
    )
    _, second_pull = jax.vjp(rms_scale, resid, moe_gain)
    resid_part, moe_gain_part = second_pull(d_mixed)
    d_resid = upstream + resid_part
    resid_b = d_resid.astype(jnp.bfloat16)
    grad_gathered = lax.all_gather(resid_b, "expert", axis=0, tiled=True)
    out_grad = contract(attended, grad_gathered, 0, 0)
    d_attended = contract(grad_gathered, w_out, 1, 1).astype(jnp.bfloat16)
    grad_blocks = d_attended.reshape(block_count, block_rows, heads_here, HEAD_DIM)

    def backward_block(totals, members):
        query_blk, grad_blk, place_blk, total_blk = members
        query_top = jnp.max(place_blk)

        def dot_step(kb, acc):

            def dot_live(total):
                key_blk, value_blk, kplace = key_piece(kb)
                scores = masked_scores(query_blk, key_blk, place_blk, kplace, score_scale)
                prob_exact = jnp.exp(scores - total_blk[:, :, None])
                d_probs = jnp.einsum(
                    "qhd,khd->hqk", grad_blk, value_blk, preferred_element_type=jnp.float32
                )
                return total + jnp.sum(prob_exact * d_probs, axis=-1)

            return lax.cond(key_lowest[kb] <= query_top, dot_live, lambda total: total, acc)

        row_dot = lax.fori_loop(
            0, key_count, dot_step, jnp.zeros((heads_here, block_rows), jnp.float32)
        )

        def grad_step(kb, carry):

            def grad_live(state):
                key_acc, value_acc, query_acc = state
                start = kb * block_rows
                key_blk, value_blk, kplace = key_piece(kb)
                scores = masked_scores(query_blk, key_blk, place_blk, kplace, score_scale)
                prob_exact = jnp.exp(scores - total_blk[:, :, None])
                prob_b = prob_exact.astype(jnp.bfloat16)
                d_probs = jnp.einsum(
                    "qhd,khd->hqk", grad_blk, value_blk, preferred_element_type=jnp.float32
                )
                d_scores = (prob_exact * (d_probs - row_dot[..., None]) * score_scale).astype(
                    jnp.bfloat16
                )
                query_acc = query_acc + jnp.einsum(
                    "hqk,khd->qhd", d_scores, key_blk, preferred_element_type=jnp.float32
                )
                key_add = jnp.einsum(
                    "hqk,qhd->khd", d_scores, query_blk, preferred_element_type=jnp.float32
                )
                value_add = jnp.einsum(
                    "hqk,qhd->khd", prob_b, grad_blk, preferred_element_type=jnp.float32
                )
                key_acc = lax.dynamic_update_slice_in_dim(
                    key_acc,
                    lax.dynamic_slice_in_dim(key_acc, start, block_rows, 0) + key_add,
                    start,
                    0,
                )
                value_acc = lax.dynamic_update_slice_in_dim(
                    value_acc,
                    lax.dynamic_slice_in_dim(value_acc, start, block_rows, 0) + value_add,
                    start,
                    0,
                )
                return (key_acc, value_acc, query_acc)

            return lax.cond(key_lowest[kb] <= query_top, grad_live, lambda state: state, carry)

        start_grad = (
            totals[0],
            totals[1],
            jnp.zeros((block_rows, heads_here, HEAD_DIM), jnp.float32),
        )
        key_acc, value_acc, d_query = lax.fori_loop(0, key_count, grad_step, start_grad)
        return ((key_acc, value_acc), d_query)

    zero_heads = jnp.zeros((seq_rows, heads_here, HEAD_DIM), jnp.float32)
    (key_acc, value_acc), d_queries = lax.scan(
        backward_block,
        (zero_heads, zero_heads),
        (query_blocks, grad_blocks, place_blocks, log_totals),
    )
    key_grad, value_grad = (
        lax.psum_scatter(
            key_acc.reshape(seq_rows, feat_width).astype(jnp.bfloat16),
            "context",
            scatter_dimension=0,
            tiled=True,
        ).astype(jnp.float32),
        lax.psum_scatter(
            value_acc.reshape(seq_rows, feat_width).astype(jnp.bfloat16),
            "context",
            scatter_dimension=0,
            tiled=True,
        ).astype(jnp.float32),
    )
    d_rotated = jnp.stack([d_queries.reshape(span_rows, feat_width), key_grad])
    _, prep_pull = jax.vjp(prep_local, projected, qk_gain)
    d_pair, qk_part = prep_pull(d_rotated)
    d_proj = jnp.concatenate([d_pair, value_grad[None]], axis=0).astype(jnp.bfloat16)
    qkv_grad = jnp.einsum("rd,krf->kdf", gathered_in, d_proj, preferred_element_type=jnp.float32)
    piece_rows = d_proj
    d_normed = lax.psum_scatter(
        jnp.einsum("krf,kdf->rd", piece_rows, w_qkv, preferred_element_type=jnp.float32).astype(
            jnp.bfloat16
        ),
        "expert",
        scatter_dimension=0,
        tiled=True,
    ).astype(jnp.float32)
    _, first_pull = jax.vjp(rms_scale, tokens, attn_gain)
    token_part, attn_gain_part = first_pull(d_normed)
    grad_in = d_resid + token_part
    qkv_sum, out_sum, qk_sum = (
        lax.psum(qkv_grad.astype(jnp.bfloat16), ("dp", "context")).astype(jnp.float32),
        lax.psum(out_grad.astype(jnp.bfloat16), ("dp", "context")).astype(jnp.float32),
        lax.psum(qk_part.astype(jnp.bfloat16), ("dp", "context")).astype(jnp.float32),
    )
    attn_sum, moe_sum, router_sum = lax.psum(
        (attn_gain_part, moe_gain_part, router_part), ("dp", "context", "expert")
    )
    return (
        hidden_out[None],
        grad_in[None],
        attn_sum,
        qkv_sum,
        qk_sum,
        out_sum,
        moe_sum,
        router_sum,
        gate_sum,
        up_sum,
        down_sum,
    )


def solution(mesh):
    grouped = mesh.shape["context"] == 4 and mesh.shape["expert"] == 4
    on_device = fast_device if grouped else portable_device
    placed = (
        P("dp", ("context", "expert"), None),
        P(),
        P(None, None, "expert"),
        P(None, "expert"),
        P("expert", None),
        P(),
        P(),
        P(("context", "expert"), None, None),
        P(("context", "expert"), None, None),
        P(("context", "expert"), None, None),
        P("dp", ("context", "expert"), None),
        P("dp", ("context", "expert"), None),
    )
    return jax.shard_map(
        on_device,
        mesh=mesh,
        in_specs=placed,
        out_specs=(
            P("dp", ("context", "expert"), None),
            P("dp", ("context", "expert"), None),
            P(),
            P(None, None, "expert"),
            P(None, "expert"),
            P("expert", None),
            P(),
            P(),
            P(("context", "expert"), "dp", None),
            P(("context", "expert"), "dp", None),
            P(("context", "expert"), "dp", None),
        ),
        check_vma=False,
    )
```
